32 devices in a mesh: section: 4 (over x, core), tensor: 2 (over y), dp: 4 (over z).
Axes of the slice: x: 2, y: 2, z: 4, core: 2. Of those that a mesh axis runs over, the one named last changes fastest.
Arguments:
- residuals: bfloat16 [4, 4, 2, 128, 8192], P('section', 'dp', None, 'tensor'), may hold values from -6 to 6
- norm_gain: bfloat16 [4, 8192], P('section'), may hold values from 0.5 to 1.5
- projection: bfloat16 [4, 8192, 2, 2, 128], P('section', None, 'tensor'), may hold values from -0.0625 to 0.0625
- queries: bfloat16 [4, 4, 2, 128, 2, 1024], P('section', 'dp', None, None, 'tensor'), may hold values from -48 to 48
- output_grad: bfloat16 [4, 4, 2, 128, 2, 1024], P('section', 'dp', None, None, 'tensor'), may hold values from -6 to 6
- section_cotangent: bfloat16 [4, 4, 128, 8192], P('section', 'dp', 'tensor'), may hold values from -6 to 6
- loss_cotangent: bfloat16 [4, 128, 8192], P('dp', 'tensor'), may hold values from -6 to 6
- lengths: int32 [4, 4, 2], P('section', 'dp'), may hold values from 64 to 128
- segments: int32 [4, 4, 2, 128], P('section', 'dp'), may hold values from 0 to 2, never falling along the last dimension, each value on 1 to 64 neighbouring positions
Outputs:
- query_grad: bfloat16 [4, 4, 2, 128, 2, 1024], P('section', 'dp', None, None, 'tensor')
- residual_grad: bfloat16 [4, 4, 128, 8192], P('section', 'dp', 'tensor')
- projection_grad: bfloat16 [4, 8192, 2, 2, 128], P('section', 'dp', 'tensor')
The draws below stay inside these ranges and needn't reach their ends.
All inputs are finite; a program needn't handle non-finite values.
Results may differ from the reference program's by a relative error of at most 0.015.
Values may be sent and summed in bfloat16 or wider, within the bound.
A program may use at most 64 MiB of HBM per device.

```python
import math
import jax
import jax.numpy as jnp
import numpy as np
from jax import lax

D = 8192
HD = 128
GROUP = 8
KVH = 2
SEQ = 128
TICKS = 2
SECTIONS = 4
REPLICAS = 4


def draw_queries(key, part):
    shape = (SECTIONS, REPLICAS, TICKS, SEQ, KVH, GROUP * HD)
    base = jnp.clip(jax.random.normal(jax.random.fold_in(key, 11), shape, jnp.float32), -6.0, 6.0)
    return base.astype(jnp.bfloat16)


def set_ends(drawn, stream_key, least, high):
    longest = drawn.shape.index(max(drawn.shape))
    spots = []
    for shift in (0, 1):
        where = [jax.random.randint(jax.random.fold_in(stream_key, axis), (), 0, length) for axis, length in enumerate(drawn.shape)]
        where[longest] = (where[longest] + shift) % drawn.shape[longest]
        spots.append(tuple(where))
    return drawn.at[spots[0]].set(least).at[spots[1]].set(high)


def steps_of(stream_key, dims, cuts, least, top_value):
    factor_of, own = 1.0, jax.random.fold_in(stream_key, 6)
    for axis_at, parts in cuts:
        heights = jnp.exp(jax.random.uniform(jax.random.fold_in(own, axis_at), (parts,), jnp.float32, least / len(cuts), top_value / len(cuts)))
        factor_of = factor_of * jnp.repeat(heights, dims[axis_at] // parts).reshape([-1 if axis == axis_at else 1 for axis in range(len(dims))])
    return factor_of


def length_profile(count, total, reach, skew):
    weights = [(1 << 20) // math.isqrt(grade ** skew) + 1 for grade in range(2, count + 1)]
    surplus, holding = total - reach - (count - 1), [1] * (count - 1)
    while surplus > 0:
        movable = [i for i in range(count - 1) if holding[i] < reach]
        whole, budget = sum([weights[i] for i in movable]), surplus
        for i in movable:
            addition = min(reach - holding[i], max(1, budget * weights[i] // whole), surplus)
            holding[i] = holding[i] + addition
            surplus = surplus - addition
    return np.array([reach] + holding)


def ragged_sizes(rng, amount, total, limit, slope):
    if amount == 2:
        one = jax.random.randint(rng, (), max(1, total - limit), min(limit, total - 1) + 1)
        return jnp.stack([one, total - one])
    tallies = jnp.asarray(length_profile(amount, total, limit, slope), jnp.int32)
    pairs = (amount - 1) // 2
    giver, taker = tallies[1:1 + 2 * pairs:2], tallies[2:2 + 2 * pairs:2]
    slack = jnp.minimum(giver - 1, limit - taker)
    shifted = jax.random.randint(jax.random.fold_in(rng, 1), (pairs,), 0, 1 << 20) % (slack + 1)
    tallies = tallies.at[1:1 + 2 * pairs:2].set(giver - shifted).at[2:2 + 2 * pairs:2].set(taker + shifted)
    return tallies[jax.random.permutation(jax.random.fold_in(rng, 2), amount)]


def scatter_about(rng, extent, deviation, most, split=(), kind=jnp.bfloat16):
    values = deviation * jax.random.normal(rng, extent, jnp.float32)
    if split:
        values = values * steps_of(rng, extent, split, -0.22, 0.18)
    return jnp.clip(values, -most, most).astype(kind)


def setup_inputs(seed: int = 0) -> dict:
    seeds = jax.random.split(jax.random.key(seed), 10)
    return {
        "residuals": scatter_about(seeds[0], (SECTIONS, REPLICAS, TICKS, SEQ, D), 1.0, 6.0, ((0, 4), (1, 4), (3, 2))),
        "norm_gain": jnp.clip(1.0 + 0.1 * jax.random.normal(seeds[1], (SECTIONS, D), jnp.float32), 0.5, 1.5).astype(jnp.bfloat16),
        "projection": scatter_about(seeds[2], (SECTIONS, D, KVH, 2, HD), D ** -0.5, 0.0625, ((0, 4), (2, 2))),
        "queries": draw_queries(jax.random.fold_in(seeds[9], 71), 0),
        "output_grad": scatter_about(seeds[4], (SECTIONS, REPLICAS, TICKS, SEQ, KVH, GROUP * HD), 1.0, 6.0, ((0, 4), (1, 4), (4, 2))),
        "section_cotangent": scatter_about(seeds[5], (SECTIONS, REPLICAS, SEQ, D), 1.0, 6.0, ((0, 4), (1, 4), (2, 2))),
        "loss_cotangent": scatter_about(seeds[6], (REPLICAS, SEQ, D), 1.0, 6.0, ((0, 4), (1, 2))),
        "lengths": set_ends(jax.random.randint(seeds[7], (SECTIONS, REPLICAS, TICKS), SEQ // 2, SEQ + 1), jax.random.fold_in(seeds[7], 1), SEQ // 2, SEQ).astype(jnp.int32),
        "segments": jax.vmap(lambda own: jnp.searchsorted(jnp.cumsum(ragged_sizes(own, 3, SEQ, SEQ // 2, 1)), jnp.arange(SEQ), side="right"))(jax.random.split(seeds[8], SECTIONS * REPLICAS * TICKS)).reshape((SECTIONS, REPLICAS, TICKS, SEQ)).astype(jnp.int32),
    }


EPSILON = 1e-05
MASKED = -1e+30

def settle(tensor):
    return lax.optimization_barrier(tensor).astype(jnp.float32)

def attend_grad(query, key_rows, value_rows, masked_grad, visible):
    scaling = HD ** (-0.5)
    query_wide = settle(query)
    key_wide = settle(key_rows)
    value_wide = settle(value_rows)
    grad_wide = settle(masked_grad)
    scores = jnp.einsum('gqd,kd->gqk', query_wide, key_wide) * scaling
    scores = jnp.where(visible[None], scores, MASKED)
    row_max = lax.optimization_barrier(jnp.max(scores, axis=-1, keepdims=True))
    exponent = jnp.exp(scores - row_max)
    attention = exponent / lax.optimization_barrier(jnp.sum(exponent, axis=-1, keepdims=True))
    attention_wide = settle(attention.astype(jnp.bfloat16))
    mixed = jnp.einsum('gqk,kd->gqd', attention_wide, value_wide)
    correction = lax.optimization_barrier(jnp.sum(grad_wide * mixed, axis=-1))
    value_grad = jnp.einsum('gqk,gqd->kd', attention_wide, grad_wide)
    weight_grad = jnp.einsum('gqd,kd->gqk', grad_wide, value_wide)
    score_grad = settle((attention * (weight_grad - correction[..., None])).astype(jnp.bfloat16))
    query_grad = (jnp.einsum('gqk,kd->gqd', score_grad, key_wide) * scaling).astype(jnp.bfloat16)
    key_grad = jnp.einsum('gqk,gqd->kd', score_grad, query_wide) * scaling
    return (query_grad, jnp.concatenate([key_grad, value_grad], axis=1).astype(jnp.bfloat16))

def section_tick(residual, gain_row, weights, query_rows, grad_rows, length, segment):
    upcast = residual.astype(jnp.float32)
    inverse = lax.rsqrt(lax.optimization_barrier(jnp.mean(upcast * upcast, axis=1, keepdims=True)) + EPSILON)
    gain_wide = gain_row.astype(jnp.float32)
    normed = (upcast * inverse * gain_wide).astype(jnp.bfloat16)
    projected = jnp.dot(normed, weights, preferred_element_type=jnp.float32).astype(jnp.bfloat16)
    projected = projected.reshape(SEQ, KVH, 2, HD)
    position = jnp.arange(SEQ, dtype=jnp.int32)
    visible = (position[None, :] <= position[:, None]) & (segment[:, None] == segment[None, :])
    live_mask = (position < length).astype(jnp.bfloat16)
    masked_grad = grad_rows * live_mask[:, None, None]
    query_heads = query_rows.reshape(SEQ, KVH, GROUP, HD).transpose(1, 2, 0, 3)
    grad_heads = masked_grad.reshape(SEQ, KVH, GROUP, HD).transpose(1, 2, 0, 3)
    key_heads = projected[:, :, 0, :].transpose(1, 0, 2)
    value_heads = projected[:, :, 1, :].transpose(1, 0, 2)
    query_grad, pair_grad = jax.vmap(attend_grad, in_axes=(0, 0, 0, 0, None))(query_heads, key_heads, value_heads, grad_heads, visible)
    query_grad = query_grad.transpose(2, 0, 1, 3).reshape(SEQ, KVH, GROUP * HD)
    head_weights = weights.astype(jnp.float32).reshape(D, KVH, 2 * HD)
    partial_value = jnp.einsum('hsc,dhc->hsd', settle(pair_grad), head_weights)
    normed_grad = lax.optimization_barrier(jnp.sum(settle(partial_value.astype(jnp.bfloat16)), axis=0))
    scaled = normed_grad * gain_wide
    norm_back = inverse * scaled - upcast * inverse * inverse * inverse * lax.optimization_barrier(jnp.mean(scaled * upcast, axis=1, keepdims=True))
    pair_flat = pair_grad.transpose(1, 0, 2).reshape(SEQ, KVH * 2 * HD)
    return (query_grad, pair_flat, normed, norm_back)

def reference(residuals, norm_gain, projection, queries, output_grad, section_cotangent, loss_cotangent, lengths, segments):

    def first_pass(section_index):
        weights = projection[section_index].reshape(D, KVH * 2 * HD)

        def replica_pass(replica):
            outcome = section_tick(residuals[section_index, replica, 0], norm_gain[section_index], weights, queries[section_index, replica, 0], output_grad[section_index, replica, 0], lengths[section_index, replica, 0], segments[section_index, replica, 0])
            return (section_cotangent[section_index, replica].astype(jnp.float32) + outcome[3]).astype(jnp.bfloat16)
        return lax.map(replica_pass, jnp.arange(REPLICAS, dtype=jnp.int32))
    outgoing = lax.map(first_pass, jnp.arange(SECTIONS, dtype=jnp.int32))
    incoming = jnp.concatenate([outgoing[1:], loss_cotangent[None]], axis=0)

    def second_pass(section_index):
        weights = projection[section_index].reshape(D, KVH * 2 * HD)

        def replica_step(running, replica):
            query_list = []
            replica_sum = jnp.zeros((D, KVH * 2 * HD), jnp.float32)
            norm_last = None
            for tick_index in range(2):
                query_grad, pair_flat, normed, norm_back = section_tick(residuals[section_index, replica, tick_index], norm_gain[section_index], weights, queries[section_index, replica, tick_index], output_grad[section_index, replica, tick_index], lengths[section_index, replica, tick_index], segments[section_index, replica, tick_index])
                query_list.append(query_grad)
                replica_sum = replica_sum + jnp.dot(normed.T, pair_flat, preferred_element_type=jnp.float32)
                norm_last = norm_back
            running = running + settle(replica_sum.astype(jnp.bfloat16))
            residual_grad = (incoming[section_index, replica].astype(jnp.float32) + norm_last).astype(jnp.bfloat16)
            return (running, (jnp.stack(query_list), residual_grad))
        running, (query_all, residual_all) = lax.scan(replica_step, jnp.zeros((D, KVH * 2 * HD), jnp.float32), jnp.arange(REPLICAS, dtype=jnp.int32))
        return (running.astype(jnp.bfloat16).reshape(D, KVH, 2, HD), query_all, residual_all)
    projection_grad, query_grad, residual_grad = lax.map(second_pass, jnp.arange(SECTIONS, dtype=jnp.int32))
    return (query_grad, residual_grad, projection_grad)
```

```python
import functools

import jax
import jax.numpy as jnp
from jax import lax
from jax.experimental import pallas as pl
from jax.experimental.pallas import tpu as pltpu
from jax.sharding import PartitionSpec as P

EPSILON = 1e-05
MASKED = -1e30
ROWS = 16
NT = (((1,), (1,)), ((), ()))
TN = (((0,), (0,)), ((), ()))


def dot(left, right, dims=(((1,), (0,)), ((), ()))):
    return lax.dot_general(left, right, dims, preferred_element_type=jnp.float32)


def kernel(
    sizes,
    x_hbm, gain_ref, w_hbm, q_hbm, og_hbm, sc_hbm, lc_hbm, len_ref, seg_ref,
    qg_hbm, rg_hbm, pg_hbm,
    x, w, q, og, sc, lc, wo, nb, inv, cols, rows_in, part_out, part_in, proj,
    pair, pairs_in, back_out, back_in, feat_out, feat_in, feat_own, total,
    sum_own, sum_out, sum_in, outgoing, incoming, qg,
    local_sem, wo_s, wo_r, col_s, col_r, row_s, row_r, part_s, part_r, pair_s, pair_r,
    back_s, back_r, feat_s, feat_r, sum_s, sum_r, out_s, out_r,
):
    S, T, N, R, D, PW, G = sizes
    HS = PW // 2
    TOK, BW = R * T, D // N
    HB = BW // 2
    section, me_t, me_n = (lax.axis_index(name) for name in ("section", "tensor", "dp"))
    scaling = HS ** (-0.5)

    def peer(k, j):
        return {"tensor": lax.rem(me_t + k, T), "dp": lax.rem(me_n + j, N)}

    def block_at(j):
        return lax.rem(me_n + j, N)

    def remote(source, target, send, receive, device):
        return pltpu.make_async_remote_copy(
            src_ref=source, dst_ref=target, send_sem=send, recv_sem=receive,
            device_id=device, device_id_type=pl.DeviceIdType.MESH,
        )

    started = []

    def start(copies):
        for copy in copies:
            copy.start()
        started.extend(copies)
        return copies

    def arrive(copies):
        for copy in copies:
            copy.wait_recv()

    pairs_of = [(x_hbm.at[0], x.at[0]), (x_hbm.at[1], x.at[1]), (w_hbm, w), (q_hbm, q), (og_hbm, og),
                (sc_hbm, sc), (lc_hbm, lc)]
    loads = [pltpu.make_async_copy(a, b, local_sem.at[i]) for i, (a, b) in enumerate(pairs_of)]
    for load in loads:
        load.start()

    barrier = pltpu.get_barrier_semaphore()
    greet = [peer(k, j) for k in range(T) for j in range(N) if (k, j) != (0, 0)]
    down = {"section": lax.rem(section + S - 1, S)}
    greet = greet + [down, {"section": lax.rem(section + 1, S)}]
    for device in greet:
        pl.semaphore_signal(barrier, 1, device_id=device, device_id_type=pl.DeviceIdType.MESH)
    pl.semaphore_wait(barrier, len(greet))

    own_rows = pl.ds(pl.multiple_of(me_n * BW, BW), BW)
    weights_sent = start([
        remote(w_hbm.at[own_rows], wo.at[k - 1], wo_s.at[k - 1], wo_r.at[k - 1], peer(k, 0))
        for k in range(1, T)
    ])

    def normalize(tick):
        def step(i, _):
            rows = pl.ds(pl.multiple_of(i * ROWS, ROWS), ROWS)
            squares = jnp.zeros((ROWS, HB), jnp.float32)
            for p in range(2 * N):
                wide = x[tick, rows, p * HB:(p + 1) * HB].astype(jnp.float32)
                squares = squares + wide * wide
            inverse = lax.rsqrt(jnp.sum(squares, axis=1, keepdims=True) / D + EPSILON)
            inv[tick, rows, :] = inverse
            for p in range(2 * N):
                here = slice(p * HB, (p + 1) * HB)
                wide = x[tick, rows, here].astype(jnp.float32)
                gain = gain_ref[:, here].astype(jnp.float32)
                nb[tick, p // 2, p % 2, rows, :] = (wide * inverse * gain).astype(jnp.bfloat16)
            return _
        lax.fori_loop(0, R // ROWS, step, 0)
        for h in range(2):
            cols[tick, h, 0] = nb[tick, me_n, h]

    def send_columns(tick, h):
        return start([
            remote(nb.at[tick, block_at(j), h], cols.at[tick, h, j],
                   col_s.at[tick, h, j - 1], col_r.at[tick, h, j - 1], peer(0, j))
            for j in range(1, N)
        ])

    loads[0].wait()
    normalize(0)
    columns_sent = {(0, h): send_columns(0, h) for h in range(2)}
    loads[1].wait()
    normalize(1)
    loads[2].wait()

    own_tokens = pl.ds(pl.multiple_of(me_t * R, R), R)

    def tokens_of(k):
        return pl.ds(pl.multiple_of(lax.rem(me_t + k, T) * R, R), R)

    def project_own(tick):
        value = jnp.zeros((R, PW), jnp.float32)
        for p in range(2 * N):
            value = value + dot(nb[tick, p // 2, p % 2], w[p * HB:(p + 1) * HB, :])
        proj[own_tokens, :] = value.astype(jnp.bfloat16)

    def send_partials(tick, halves):
        sent = []
        for k in range(1, T):
            value = sum(
                dot(cols[tick, h].reshape(N * R, HB), wo[k - 1, h * HB:(h + 1) * HB, :]) for h in halves
            )
            part_out[tick, k - 1] = value.astype(jnp.bfloat16).reshape(N, R, PW)
            sent += [
                remote(part_out.at[tick, k - 1, j], part_in.at[tick, k - 1, j],
                       part_s.at[tick, k - 1, j], part_r.at[tick, k - 1, j], peer(T - k, N - j))
                for j in range(N)
            ]
        return start(sent)

    def gather_projected(tick, cross):
        project_own(tick)
        for k in range(1, T):
            value = jnp.sum(part_in[tick, k - 1].astype(jnp.float32), axis=0)
            if cross:
                for b in range(N):
                    value = value + dot(rows_in[T - k - 1, b], w[b * BW + HB:(b + 1) * BW, :])
            proj[tokens_of(k), :] = value.astype(jnp.bfloat16)

    position_q = lax.broadcasted_iota(jnp.int32, (TOK, TOK), 0)
    position_k = lax.broadcasted_iota(jnp.int32, (TOK, TOK), 1)

    def attend(tick):
        segment = jnp.broadcast_to(seg_ref[tick:tick + 1, :].astype(jnp.float32), (TOK, TOK))
        visible = (position_k <= position_q) & (segment == segment.T)
        live = lax.broadcasted_iota(jnp.int32, (TOK, HS), 0) < len_ref[tick]
        keys, values = proj[:, :HS], proj[:, HS:]
        key_grad = jnp.zeros((TOK, HS), jnp.float32)
        value_grad = jnp.zeros((TOK, HS), jnp.float32)
        for g in range(G):
            head = slice(g * HS, (g + 1) * HS)
            query = q[tick, :, head]
            masked = jnp.where(live, og[tick, :, head], jnp.zeros((), jnp.bfloat16))
            scores = jnp.where(visible, dot(query, keys, NT) * scaling, MASKED)
            exponent = jnp.exp(scores - jnp.max(scores, axis=1, keepdims=True))
            attention = exponent * (1.0 / jnp.sum(exponent, axis=1, keepdims=True))
            low = attention.astype(jnp.bfloat16)
            mixed = dot(low, values)
            correction = jnp.sum(mixed * masked.astype(jnp.float32), axis=1, keepdims=True)
            value_grad = value_grad + dot(low, masked, TN)
            weight_grad = dot(masked, values, NT)
            score_grad = (attention * (weight_grad - correction)).astype(jnp.bfloat16)
            qg[tick, :, head] = (dot(score_grad, keys) * scaling).astype(jnp.bfloat16)
            key_grad = key_grad + dot(score_grad, query, TN)
        pair[tick, :, :HS] = (key_grad * scaling).astype(jnp.bfloat16)
        pair[tick, :, HS:] = value_grad.astype(jnp.bfloat16)

    def send_pairs(tick):
        pairs_in[tick, 0, 0] = pair[tick, own_tokens, :]
        return start([
            remote(pair.at[tick, tokens_of(k)], pairs_in.at[tick, k, j],
                   pair_s.at[tick, k, j], pair_r.at[tick, k, j], peer(k, j))
            for j in range(N) for k in range(T) if (k, j) != (0, 0)
        ])

    def weights_of(k, columns):
        return w[pl.ds(pl.multiple_of(me_n * BW + columns.start, CH), columns.stop - columns.start), :] \
            if k == 0 else wo[k - 1, columns, :]

    CH = min(BW, 512)

    def send_back(tick, j):
        b = block_at(j)
        for c in range(0, BW, CH):
            rows = pl.ds(pl.multiple_of(b * BW + c, CH), CH)
            value = dot(pair[tick], w[rows, :], NT).astype(jnp.bfloat16)
            back_out[j - 1, :, :, c:c + CH] = value.reshape(T, R, CH)
        return start([
            remote(back_out.at[j - 1, lax.rem(me_t + k, T)], back_in.at[j - 1, k - 1],
                   back_s.at[j - 1, k - 1], back_r.at[j - 1, k - 1], peer(k, 0))
            for k in range(1, T)
        ])

    def own_feature_grad(tick):
        for c in range(0, BW, CH):
            here = slice(c, c + CH)
            value = jnp.zeros((R, CH), jnp.float32)
            for k in range(T):
                weights = weights_of(k, here)
                term = dot(pairs_in[tick, k, 0], weights, NT)
                value = value + term.astype(jnp.bfloat16).astype(jnp.float32)
            feat_own[:, here] = value

    def send_features(tick):
        sent = []
        for c in range(0, BW, CH):
            here = slice(c, c + CH)
            value = jnp.zeros((N * R, CH), jnp.float32)
            for k in range(T):
                term = dot(pairs_in[tick, k].reshape(N * R, PW), weights_of(k, here), NT)
                value = value + term.astype(jnp.bfloat16).astype(jnp.float32)
            feat_own[:, here] = value[:R]
            feat_out[:, :, here] = value[R:].astype(jnp.bfloat16).reshape(N - 1, R, CH)
        return start([
            remote(feat_out.at[j - 1], feat_in.at[j - 1], feat_s.at[j - 1], feat_r.at[j - 1], peer(0, N - j))
            for j in range(1, N)
        ])

    def norm_back(tick, base, target):
        def step(i, _):
            rows = pl.ds(pl.multiple_of(i * ROWS, ROWS), ROWS)
            inverse = inv[tick, rows, :]
            products = jnp.zeros((ROWS, BW), jnp.float32)
            for b in range(N):
                here = slice(b * BW, (b + 1) * BW)
                scaled = total[b, rows, :] * gain_ref[:, here].astype(jnp.float32)
                products = products + scaled * x[tick, rows, here].astype(jnp.float32)
            mean = jnp.sum(products, axis=1, keepdims=True) / D
            cube = inverse * inverse * inverse * mean
            for b in range(N):
                here = slice(b * BW, (b + 1) * BW)
                scaled = total[b, rows, :] * gain_ref[:, here].astype(jnp.float32)
                back = inverse * scaled - x[tick, rows, here].astype(jnp.float32) * cube
                target[rows, here] = (base(rows, here) + back).astype(jnp.bfloat16)
            return _
        lax.fori_loop(0, R // ROWS, step, 0)

    def accumulate(tick, k, first):
        right = pairs_in[tick, k].reshape(N * R, PW)
        for h in range(2):
            value = dot(cols[tick, h].reshape(N * R, HB), right, TN)
            here = slice(h * HB, (h + 1) * HB)
            sum_own[k, here, :] = value if first else sum_own[k, here, :] + value

    arrive(weights_sent)
    arrive(columns_sent[0, 0])
    arrive(columns_sent[0, 1])
    partials = [send_partials(0, (0, 1))]
    columns_sent[1, 0] = send_columns(1, 0)
    rows_sent = start([
        remote(nb.at[1, :, 1], rows_in.at[k - 1], row_s.at[k - 1], row_r.at[k - 1], peer(k, 0))
        for k in range(1, T)
    ])
    loads[3].wait()
    loads[4].wait()
    arrive(partials[0])
    gather_projected(0, False)
    attend(0)
    pairs_sent = [send_pairs(0)]

    arrive(columns_sent[1, 0])
    partials.append(send_partials(1, (0,)))
    columns_sent[1, 1] = send_columns(1, 1)
    backs_sent = [send_back(0, j) for j in range(1, N - 1)]
    arrive(pairs_sent[0])
    own_feature_grad(0)
    for k in range(T):
        accumulate(0, k, True)
    arrive(rows_sent)
    arrive(partials[1])
    gather_projected(1, True)
    attend(1)
    pairs_sent.append(send_pairs(1))
    backs_sent.append(send_back(0, N - 1))
    query_out = pltpu.make_async_copy(qg, qg_hbm, local_sem.at[3])
    query_out.start()

    arrive(pairs_sent[1])
    total[me_n] = feat_own[...]
    features_sent = send_features(1)
    arrive(columns_sent[1, 1])
    sums_sent = []
    for k in range(1, T):
        accumulate(1, k, False)
        sum_out[k - 1] = sum_own[k].astype(jnp.bfloat16)
        sums_sent += start([
            remote(sum_out.at[k - 1], sum_in.at[k - 1], sum_s.at[k - 1], sum_r.at[k - 1], peer(T - k, 0))
        ])
    accumulate(1, 0, False)

    for j in range(1, N):
        arrive(backs_sent[j - 1])
        value = back_out[j - 1, me_t].astype(jnp.float32)
        for k in range(1, T):
            value = value + back_in[j - 1, k - 1].astype(jnp.float32)
        total[block_at(j)] = value
    loads[5].wait()
    loads[6].wait()
    norm_back(0, lambda rows, here: sc[rows, here].astype(jnp.float32), outgoing)
    shift = start([remote(outgoing, incoming, out_s.at[0], out_r.at[0], down)])

    total[me_n] = feat_own[...]
    for j in range(1, N):
        arrive([features_sent[j - 1]])
        total[block_at(j)] = feat_in[j - 1].astype(jnp.float32)
    arrive(shift)
    is_last = section == S - 1

    def arriving(rows, here):
        return jnp.where(is_last, lc[rows, here].astype(jnp.float32), incoming[rows, here].astype(jnp.float32))

    for copy in shift:
        copy.wait_send()
    norm_back(1, arriving, outgoing)
    residual_out = pltpu.make_async_copy(outgoing, rg_hbm, local_sem.at[0])
    residual_out.start()

    for copy in sums_sent:
        copy.wait()
    final = sum_own[0]
    for k in range(1, T):
        final = final + sum_in[k - 1].astype(jnp.float32)
    sum_out[0] = final.astype(jnp.bfloat16)
    weight_out = pltpu.make_async_copy(sum_out.at[0], pg_hbm, local_sem.at[1])
    weight_out.start()
    for copy in started:
        if not any(copy is other for other in shift + sums_sent):
            copy.wait_send()
    query_out.wait()
    residual_out.wait()
    weight_out.wait()


def on_device(residuals, norm_gain, projection, queries, output_grad, section_cotangent, loss_cotangent, lengths, segments):
    x, q, og = residuals[0, 0], queries[0, 0, :, :, 0, :], output_grad[0, 0, :, :, 0, :]
    ticks, R, D = x.shape
    PW = 2 * projection.shape[4]
    S, T, N = (lax.axis_size(name) for name in ("section", "tensor", "dp"))
    TOK, BW, HB = R * T, D // N, D // N // 2
    sizes = (S, T, N, R, D, PW, q.shape[-1] // (PW // 2))
    low, wide, dma = jnp.bfloat16, jnp.float32, pltpu.SemaphoreType.DMA
    anywhere, vmem = pl.BlockSpec(memory_space=pl.ANY), pl.BlockSpec(memory_space=pltpu.VMEM)
    outs = pl.pallas_call(
        functools.partial(kernel, sizes),
        out_shape=(
            jax.ShapeDtypeStruct(q.shape, low),
            jax.ShapeDtypeStruct((R, D), low),
            jax.ShapeDtypeStruct((BW, PW), low),
        ),
        in_specs=[anywhere, vmem] + [anywhere] * 5 + [pl.BlockSpec(memory_space=pltpu.SMEM), vmem],
        out_specs=[anywhere] * 3,
        scratch_shapes=[
            pltpu.VMEM(x.shape, low), pltpu.VMEM((D, PW), low), pltpu.VMEM(q.shape, low), pltpu.VMEM(q.shape, low),
            pltpu.VMEM((R, D), low), pltpu.VMEM((R, D), low),
            pltpu.VMEM((T - 1, BW, PW), low),
            pltpu.VMEM((ticks, N, 2, R, HB), low), pltpu.VMEM((ticks, R, 1), wide),
            pltpu.VMEM((ticks, 2, N, R, HB), low), pltpu.VMEM((T - 1, N, R, HB), low),
            pltpu.VMEM((ticks, T - 1, N, R, PW), low), pltpu.VMEM((ticks, T - 1, N, R, PW), low),
            pltpu.VMEM((TOK, PW), low),
            pltpu.VMEM((ticks, TOK, PW), low), pltpu.VMEM((ticks, T, N, R, PW), low),
            pltpu.VMEM((N - 1, T, R, BW), low), pltpu.VMEM((N - 1, T - 1, R, BW), low),
            pltpu.VMEM((N - 1, R, BW), low), pltpu.VMEM((N - 1, R, BW), low), pltpu.VMEM((R, BW), wide),
            pltpu.VMEM((N, R, BW), wide),
            pltpu.VMEM((T, BW, PW), wide), pltpu.VMEM((T - 1, BW, PW), low), pltpu.VMEM((T - 1, BW, PW), low),
            pltpu.VMEM((R, D), low), pltpu.VMEM((R, D), low), pltpu.VMEM(q.shape, low),
            dma((7,)), dma((T - 1,)), dma((T - 1,)),
            dma((ticks, 2, N - 1)), dma((ticks, 2, N - 1)), dma((T - 1,)), dma((T - 1,)),
            dma((ticks, T - 1, N)), dma((ticks, T - 1, N)), dma((ticks, T, N)), dma((ticks, T, N)),
            dma((N - 1, T - 1)), dma((N - 1, T - 1)), dma((N - 1,)), dma((N - 1,)),
            dma((T - 1,)), dma((T - 1,)), dma((1,)), dma((1,)),
        ],
        compiler_params=pltpu.CompilerParams(
            collective_id=0, has_side_effects=True, vmem_limit_bytes=62_000_000
        ),
    )(
        x, norm_gain, projection.reshape(D, PW), q, og, section_cotangent[0, 0], loss_cotangent[0],
        lengths.reshape(ticks), segments[0, 0],
    )
    query_grad, residual_grad, projection_grad = outs
    return (
        query_grad[None, None, :, :, None, :],
        residual_grad[None, None],
        projection_grad.reshape(1, BW, 1, 2, PW // 2),
    )


def solution(mesh):
    in_specs = (
        P("section", "dp", None, "tensor", None),
        P("section", None),
        P("section", None, "tensor", None, None),
        P("section", "dp", None, None, "tensor", None),
        P("section", "dp", None, None, "tensor", None),
        P("section", "dp", "tensor", None),
        P("dp", "tensor", None),
        P("section", "dp", None),
        P("section", "dp", None, None),
    )
    out_specs = (
        P("section", "dp", None, None, "tensor", None),
        P("section", "dp", "tensor", None),
        P("section", "dp", "tensor", None, None),
    )
    return jax.shard_map(on_device, mesh=mesh, in_specs=in_specs, out_specs=out_specs, check_vma=False)
```

```python
import functools

import jax
import jax.numpy as jnp
from jax import lax
from jax.experimental import pallas as pl
from jax.experimental.pallas import tpu as pltpu
from jax.sharding import PartitionSpec as P

EPSILON = 1e-05
MASKED = -1e30
ROWS = 16
NT = (((1,), (1,)), ((), ()))
TN = (((0,), (0,)), ((), ()))


def dot(left, right, dims=(((1,), (0,)), ((), ()))):
    return lax.dot_general(left, right, dims, preferred_element_type=jnp.float32)


def kernel(
    sizes,
    x_hbm, gain_ref, w_hbm, q_hbm, og_hbm, sc_hbm, lc_hbm, len_ref, seg_ref,
    qg_hbm, rg_hbm, pg_hbm,
    x, raw, w, q, og, sc, lc, wo, nb, inv, cols, rows_in, part_out, part_in, part_sum, part_all, proj,
    pair, pairs_in, back_out, back_in, feat_out, feat_in, feat_own, total,
    sum_own, sum_out, sum_in, outgoing, incoming, result, qg, pg, stacked, score_grads,
    local_sem, raw_sem, wo_s, wo_r, col_s, col_r, row_s, row_r, part_s, part_r, psum_s, psum_r,
    pair_s, pair_r, pair_fs, pair_fr, back_s, back_r, feat_s, feat_r, sum_s, sum_r, out_s, out_r,
):
    S, T, N, R, D, PW, G = sizes
    HS = PW // 2
    TOK, BW = R * T, D // N
    HB = BW // 2
    WR = min(BW, 256)
    section, me_t, me_n = (lax.axis_index(name) for name in ("section", "tensor", "dp"))
    scaling = HS ** (-0.5)

    paired = N & (N - 1) == 0

    def block_at(j):
        if not paired:
            return lax.rem(me_n + j, N)
        at = me_n
        for bit in range(j.bit_length()):
            if j >> bit & 1:
                at = at + (1 << bit) * (1 - 2 * lax.rem(lax.div(me_n, 1 << bit), 2))
        return at

    def peer(k, j):
        return {"tensor": lax.rem(me_t + k, T), "dp": block_at(j)}

    def reverse(j):
        return j if paired else (N - j) % N

    def remote(source, target, send, receive, device):
        return pltpu.make_async_remote_copy(
            src_ref=source, dst_ref=target, send_sem=send, recv_sem=receive,
            device_id=device, device_id_type=pl.DeviceIdType.MESH,
        )

    started = []

    def start(copies):
        for copy in copies:
            copy.start()
        started.extend(copies)
        return copies

    def arrive(copies):
        for copy in copies:
            copy.wait_recv()

    own_rows = pl.ds(pl.multiple_of(me_n * BW, BW), BW)

    def weight_rows(j):
        return pl.ds(pl.multiple_of(block_at(j) * BW, BW), BW)

    raw_loads = [
        pltpu.make_async_copy(w_hbm.at[weight_rows(j)], raw.at[weight_rows(j)], raw_sem.at[j]) for j in range(N)
    ]
    pairs_of = [(x_hbm.at[0], x.at[0]), (x_hbm.at[1], x.at[1]), (q_hbm, q), (og_hbm, og), (sc_hbm, sc), (lc_hbm, lc)]
    loads = [pltpu.make_async_copy(a, b, local_sem.at[i]) for i, (a, b) in enumerate(pairs_of)]
    for load in loads[:1] + raw_loads[:1] + loads[1:2] + raw_loads[1:] + loads[2:]:
        load.start()

    barrier = pltpu.get_barrier_semaphore()
    greet = [peer(k, 0) for k in range(1, T)] + [peer(0, j) for j in range(1, N)]
    down = {"section": lax.rem(section + S - 1, S)}
    greet = greet + [down, {"section": lax.rem(section + 1, S)}]
    for device in greet:
        pl.semaphore_signal(barrier, 1, device_id=device, device_id_type=pl.DeviceIdType.MESH)

    def place_weights(j):
        raw_loads[j].wait()
        first = block_at(j) * BW

        def step(i, _):
            rows = pl.ds(pl.multiple_of(first + i * WR, WR), WR)
            w[rows, :] = raw[rows].reshape(WR, PW)
            return _
        lax.fori_loop(0, BW // WR, step, 0)

    def normalize(tick):
        def step(i, _):
            rows = pl.ds(pl.multiple_of(i * ROWS, ROWS), ROWS)
            squares = jnp.zeros((ROWS, HB), jnp.float32)
            for p in range(2 * N):
                wide = x[tick, rows, p * HB:(p + 1) * HB].astype(jnp.float32)
                squares = squares + wide * wide
            inverse = lax.rsqrt(jnp.sum(squares, axis=1, keepdims=True) / D + EPSILON)
            inv[tick, rows, :] = inverse
            for p in range(2 * N):
                here = slice(p * HB, (p + 1) * HB)
                wide = x[tick, rows, here].astype(jnp.float32)
                gain = gain_ref[:, here].astype(jnp.float32)
                nb[tick, p // 2, p % 2, rows, :] = (wide * inverse * gain).astype(jnp.bfloat16)
            return _
        lax.fori_loop(0, R // ROWS, step, 0)
        for h in range(2):
            cols[tick, h, 0] = nb[tick, me_n, h]

    def send_columns(tick, h, offsets=range(1, N)):
        return start([
            remote(nb.at[tick, block_at(j), h], cols.at[tick, h, j],
                   col_s.at[tick, h, j - 1], col_r.at[tick, h, j - 1], peer(0, j))
            for j in offsets
        ])

    own_tokens = pl.ds(pl.multiple_of(me_t * R, R), R)

    def tokens_of(k):
        return pl.ds(pl.multiple_of(lax.rem(me_t + k, T) * R, R), R)

    def project_own(tick):
        value = jnp.zeros((R, PW), jnp.float32)
        for p in range(2 * N):
            value = value + dot(nb[tick, p // 2, p % 2], w[p * HB:(p + 1) * HB, :])
        proj[tick, own_tokens, :] = value.astype(jnp.bfloat16)

    def send_partials(tick, halves):
        for k in range(1, T):
            value = sum(
                dot(cols[tick, h].reshape(N * R, HB), wo[k - 1, h * HB:(h + 1) * HB, :]) for h in halves
            )
            part_out[tick, :, k - 1] = value.astype(jnp.bfloat16).reshape(N, R, PW)
        return start([
            remote(part_out.at[tick, j], part_in.at[tick, j - 1],
                   part_s.at[tick, j - 1], part_r.at[tick, j - 1], peer(0, reverse(j)))
            for j in range(1, N)
        ])

    def send_part_sums(tick):
        value = part_out[tick, 0].astype(jnp.float32)
        for j in range(1, N):
            value = value + part_in[tick, j - 1].astype(jnp.float32)
        part_sum[tick] = value.astype(jnp.bfloat16)
        return start([
            remote(part_sum.at[tick, k - 1], part_all.at[tick, k - 1],
                   psum_s.at[tick, k - 1], psum_r.at[tick, k - 1], peer(T - k, 0))
            for k in range(1, T)
        ])

    def send_rows(piece):
        blocks = pl.ds(piece * (N // 2), N // 2)
        return start([
            remote(nb.at[1, blocks, 1], rows_in.at[k - 1, blocks], row_s.at[k - 1, piece], row_r.at[k - 1, piece], peer(k, 0))
            for k in range(1, T)
        ])

    def gather_projected(tick, cross):
        for k in range(1, T):
            value = part_all[tick, k - 1].astype(jnp.float32)
            if cross:
                for b in range(N):
                    value = value + dot(rows_in[T - k - 1, b], w[b * BW + HB:(b + 1) * BW, :])
            proj[tick, tokens_of(k), :] = value.astype(jnp.bfloat16)

    position_q = lax.broadcasted_iota(jnp.int32, (TOK, TOK), 0)
    position_k = lax.broadcasted_iota(jnp.int32, (TOK, TOK), 1)

    def stack_heads(tick):
        live = lax.broadcasted_iota(jnp.int32, (TOK, HS), 0) < len_ref[tick]
        for g in range(G):
            rows, head = slice(g * TOK, (g + 1) * TOK), slice(g * HS, (g + 1) * HS)
            stacked[tick, 0, rows, :] = q[tick, :, head]
            stacked[tick, 1, rows, :] = jnp.where(live, og[tick, :, head], jnp.zeros((), jnp.bfloat16))

    def attend(tick):
        segment = jnp.broadcast_to(seg_ref[tick:tick + 1, :].astype(jnp.float32), (TOK, TOK))
        visible = (position_k <= position_q) & (segment == segment.T)
        keys, values = proj[tick, :, :HS], proj[tick, :, HS:]
        query, masked = stacked[tick, 0], stacked[tick, 1]
        scores = (dot(query, keys, NT) * scaling).reshape(G, TOK, TOK)
        scores = jnp.where(visible[None], scores, MASKED)
        weight_grad = dot(masked, values, NT).reshape(G, TOK, TOK)
        exponent = jnp.exp(scores - jnp.max(scores, axis=2, keepdims=True))
        attention = exponent * (1.0 / jnp.sum(exponent, axis=2, keepdims=True))
        low = attention.astype(jnp.bfloat16).reshape(G * TOK, TOK)
        mixed = dot(low, values)
        correction = jnp.sum(mixed * masked.astype(jnp.float32), axis=1, keepdims=True).reshape(G, TOK, 1)
        score_grad = (attention * (weight_grad - correction)).astype(jnp.bfloat16).reshape(G * TOK, TOK)
        pair[tick, :, HS:] = dot(low, masked, TN).astype(jnp.bfloat16)
        pair[tick, :, :HS] = (dot(score_grad, query, TN) * scaling).astype(jnp.bfloat16)
        score_grads[tick] = score_grad

    def finish_queries(tick):
        value = (dot(score_grads[tick], proj[tick, :, :HS]) * scaling).astype(jnp.bfloat16)
        for g in range(G):
            qg[tick, :, g * HS:(g + 1) * HS] = value[g * TOK:(g + 1) * TOK]

    def send_pairs(tick):
        pairs_in[tick, 0, 0] = pair[tick, own_tokens, :]
        return start([
            remote(pair.at[tick, tokens_of(k)], pairs_in.at[tick, 0, k],
                   pair_s.at[tick, k - 1], pair_r.at[tick, k - 1], peer(k, 0))
            for k in range(1, T)
        ])

    def forward_pairs(ticks, heads, slot, offsets=range(1, N)):
        return {
            j: start([
                remote(pairs_in.at[ticks, 0, heads], pairs_in.at[ticks, j, heads],
                       pair_fs.at[slot, j - 1], pair_fr.at[slot, j - 1], peer(0, j))
            ])
            for j in offsets
        }

    def pairs_of_head(tick, k):
        return pairs_in[tick, :, k].reshape(N * R, PW)

    def weights_of(k, columns):
        return w[pl.ds(pl.multiple_of(me_n * BW + columns.start, CH), columns.stop - columns.start), :] \
            if k == 0 else wo[k - 1, columns, :]

    CH = min(BW, 512)

    def send_back(tick, j):
        b = block_at(j)
        for c in range(0, BW, CH):
            rows = pl.ds(pl.multiple_of(b * BW + c, CH), CH)
            value = dot(pair[tick], w[rows, :], NT).astype(jnp.bfloat16)
            back_out[tick, j - 1, :, :, c:c + CH] = value.reshape(T, R, CH)
        return start([
            remote(back_out.at[tick, j - 1, lax.rem(me_t + k, T)], back_in.at[tick, j - 1, k - 1],
                   back_s.at[tick, j - 1, k - 1], back_r.at[tick, j - 1, k - 1], peer(k, 0))
            for k in range(1, T)
        ])

    def feature_grads(tick, slots):
        for c in range(0, BW, CH):
            here = slice(c, c + CH)
            value = jnp.zeros((slots * R, CH), jnp.float32)
            for k in range(T):
                pairs = pairs_in[tick, :slots, k].reshape(slots * R, PW)
                term = dot(pairs, weights_of(k, here), NT)
                value = value + term.astype(jnp.bfloat16).astype(jnp.float32)
            feat_own[tick, :, here] = value[:R]
            feat_out[tick, :slots - 1, :, here] = value[R:].astype(jnp.bfloat16).reshape(slots - 1, R, CH)

    def send_features(tick, offsets):
        return {
            j: start([
                remote(feat_out.at[tick, j - 1], feat_in.at[tick, j - 1],
                       feat_s.at[tick, j - 1], feat_r.at[tick, j - 1], peer(0, reverse(j)))
            ])
            for j in offsets
        }

    def collect(tick, backs, features):
        total[me_n] = feat_own[tick]
        for j in backs:
            arrive(backs[j])
            value = back_out[tick, j - 1, me_t].astype(jnp.float32)
            for k in range(1, T):
                value = value + back_in[tick, j - 1, k - 1].astype(jnp.float32)
            total[block_at(j)] = value
        for j in features:
            arrive(features[j])
            total[block_at(j)] = feat_in[tick, j - 1].astype(jnp.float32)

    def norm_back(tick, base, target):
        def step(i, _):
            rows = pl.ds(pl.multiple_of(i * ROWS, ROWS), ROWS)
            inverse = inv[tick, rows, :]
            products = jnp.zeros((ROWS, BW), jnp.float32)
            for b in range(N):
                here = slice(b * BW, (b + 1) * BW)
                scaled = total[b, rows, :] * gain_ref[:, here].astype(jnp.float32)
                products = products + scaled * x[tick, rows, here].astype(jnp.float32)
            mean = jnp.sum(products, axis=1, keepdims=True) / D
            cube = inverse * inverse * inverse * mean
            for b in range(N):
                here = slice(b * BW, (b + 1) * BW)
                scaled = total[b, rows, :] * gain_ref[:, here].astype(jnp.float32)
                back = inverse * scaled - x[tick, rows, here].astype(jnp.float32) * cube
                target[rows, here] = (base(rows, here) + back).astype(jnp.bfloat16)
            return _
        lax.fori_loop(0, R // ROWS, step, 0)

    def accumulate(k, h):
        here = slice(h * HB, (h + 1) * HB)
        value = sum(dot(cols[tick, h].reshape(N * R, HB), pairs_of_head(tick, k), TN) for tick in range(2))
        if k == 0:
            sum_own[here, :] = value
        else:
            sum_out[k - 1, here, :] = value.astype(jnp.bfloat16)

    by_tensor = [list(range(2, N)), [N // 2]]
    by_dp = [[j for j in range(1, N) if j not in by_tensor[tick]] for tick in range(2)]

    loads[0].wait()
    normalize(0)
    pl.semaphore_wait(barrier, len(greet))
    columns_sent = {(0, h): send_columns(0, h) for h in range(2)}
    place_weights(0)
    weights_sent = start([
        remote(w.at[own_rows], wo.at[k - 1], wo_s.at[k - 1], wo_r.at[k - 1], peer(k, 0)) for k in range(1, T)
    ])
    loads[1].wait()
    normalize(1)
    rows_sent = send_rows(0)
    for j in range(1, N):
        place_weights(j)
    for tick in range(2):
        project_own(tick)
    for load in loads[2:4]:
        load.wait()
    for tick in range(2):
        stack_heads(tick)

    arrive(weights_sent)
    arrive(columns_sent[0, 0])
    arrive(columns_sent[0, 1])
    near, far = range(1, 2), range(2, N)
    partials = send_partials(0, (0, 1))
    columns_sent[1, 0] = send_columns(1, 0, near)
    columns_sent[1, 0] = columns_sent[1, 0] + send_columns(1, 0, far)
    arrive(partials)
    part_sums = [send_part_sums(0)]
    rows_sent = rows_sent + send_rows(1)
    arrive(part_sums[0])
    gather_projected(0, False)
    attend(0)
    pairs_sent = send_pairs(0)
    backs = [{}, {}]
    first, *rest = by_tensor[0]
    backs[0][first] = send_back(0, first)
    arrive(columns_sent[1, 0])
    partials = send_partials(1, (0,))
    columns_sent[1, 1] = send_columns(1, 1, near)
    columns_sent[1, 1] = columns_sent[1, 1] + send_columns(1, 1, far)
    finish_queries(0)
    arrive(partials)
    part_sums.append(send_part_sums(1))
    arrive(pairs_sent)
    everyone, others, own_head = pl.ds(0, T), pl.ds(1, T - 1), pl.ds(0, 1)
    near_moved = forward_pairs(pl.ds(0, 1), everyone, 0, near)
    others_moved = [forward_pairs(pl.ds(0, 1), others, 0, far)]
    for j in rest:
        backs[0][j] = send_back(0, j)
    arrive(rows_sent)
    arrive(part_sums[1])
    gather_projected(1, True)
    attend(1)
    pairs_sent = send_pairs(1)
    finish_queries(1)
    query_out = pltpu.make_async_copy(qg, qg_hbm, local_sem.at[2])
    query_out.start()
    arrive(near_moved[1])
    feature_grads(0, 2)
    features = [send_features(0, near)]
    arrive(pairs_sent)
    others_moved.append(forward_pairs(pl.ds(1, 1), others, 1))
    late_moved = [forward_pairs(pl.ds(1, 1), own_head, 2), forward_pairs(pl.ds(0, 1), own_head, 3, far)]
    for j in by_tensor[1]:
        backs[1][j] = send_back(1, j)

    for moved in others_moved:
        for j in moved:
            arrive(moved[j])
    arrive(columns_sent[1, 1])
    sums_sent = []
    for k in range(1, T):
        for h in range(2):
            here = pl.ds(h * HB, HB)
            accumulate(k, h)
            sums_sent += start([
                remote(sum_out.at[k - 1, here], sum_in.at[k - 1, here],
                       sum_s.at[k - 1, h], sum_r.at[k - 1, h], peer(T - k, 0))
            ])

    collect(0, backs[0], features[0])
    loads[4].wait()
    loads[5].wait()
    norm_back(0, lambda rows, here: sc[rows, here].astype(jnp.float32), outgoing)
    shift = start([remote(outgoing, incoming, out_s.at[0], out_r.at[0], down)])
    for moved in late_moved:
        for j in moved:
            arrive(moved[j])
    feature_grads(1, N)
    features.append(send_features(1, by_dp[1]))
    for h in range(2):
        accumulate(0, h)

    collect(1, backs[1], features[1])
    arrive(shift)
    is_last = section == S - 1

    def arriving(rows, here):
        return jnp.where(is_last, lc[rows, here].astype(jnp.float32), incoming[rows, here].astype(jnp.float32))

    norm_back(1, arriving, result)
    residual_out = pltpu.make_async_copy(result, rg_hbm, local_sem.at[0])
    residual_out.start()

    arrive(sums_sent)

    def finish(i, _):
        rows = pl.ds(pl.multiple_of(i * WR, WR), WR)
        final = sum_own[rows, :]
        for k in range(1, T):
            final = final + sum_in[k - 1, rows, :].astype(jnp.float32)
        pg[rows] = final.astype(jnp.bfloat16).reshape(WR, 2, HS)
        return _

    lax.fori_loop(0, BW // WR, finish, 0)
    weight_out = pltpu.make_async_copy(pg, pg_hbm, local_sem.at[1])
    weight_out.start()
    for copy in started:
        copy.wait_send()
    query_out.wait()
    residual_out.wait()
    weight_out.wait()


def copies(*refs):
    count = (len(refs) - 1) // 3
    sources, targets, held, sems = refs[:count], refs[count:2 * count], refs[2 * count:3 * count], refs[-1]
    moves = [
        [pltpu.make_async_copy(source, buffer, sems.at[i, 0]), pltpu.make_async_copy(buffer, target, sems.at[i, 1])]
        for i, (source, target, buffer) in enumerate(zip(sources, targets, held))
    ]
    for inward, _ in moves:
        inward.start()
    for inward, outward in moves:
        inward.wait()
        outward.start()
    for _, outward in moves:
        outward.wait()


def settle(arrays):
    anywhere = pl.BlockSpec(memory_space=pl.ANY)
    return pl.pallas_call(
        copies,
        out_shape=tuple(jax.ShapeDtypeStruct(array.shape, array.dtype) for array in arrays),
        in_specs=[anywhere] * len(arrays),
        out_specs=[anywhere] * len(arrays),
        scratch_shapes=[pltpu.VMEM(array.shape, array.dtype) for array in arrays] + [pltpu.SemaphoreType.DMA((len(arrays), 2))],
    )(*arrays)


def on_device(residuals, norm_gain, projection, queries, output_grad, section_cotangent, loss_cotangent, lengths, segments):
    x, q, og = residuals[0, 0], queries[0, 0, :, :, 0, :], output_grad[0, 0, :, :, 0, :]
    ticks, R, D = x.shape
    PW = 2 * projection.shape[4]
    S, T, N = (lax.axis_size(name) for name in ("section", "tensor", "dp"))
    TOK, BW, HB = R * T, D // N, D // N // 2
    sizes = (S, T, N, R, D, PW, q.shape[-1] // (PW // 2))
    low, wide, dma = jnp.bfloat16, jnp.float32, pltpu.SemaphoreType.DMA
    anywhere, vmem = pl.BlockSpec(memory_space=pl.ANY), pl.BlockSpec(memory_space=pltpu.VMEM)
    outs = pl.pallas_call(
        functools.partial(kernel, sizes),
        out_shape=(
            jax.ShapeDtypeStruct(q.shape, low),
            jax.ShapeDtypeStruct((R, D), low),
            jax.ShapeDtypeStruct((BW, 2, PW // 2), low),
        ),
        in_specs=[anywhere, vmem] + [anywhere] * 5 + [pl.BlockSpec(memory_space=pltpu.SMEM), vmem],
        out_specs=[anywhere] * 3,
        scratch_shapes=[
            pltpu.VMEM(x.shape, low), pltpu.VMEM((D, 2, PW // 2), low), pltpu.VMEM((D, PW), low), pltpu.VMEM(q.shape, low), pltpu.VMEM(q.shape, low),
            pltpu.VMEM((R, D), low), pltpu.VMEM((R, D), low),
            pltpu.VMEM((T - 1, BW, PW), low),
            pltpu.VMEM((ticks, N, 2, R, HB), low), pltpu.VMEM((ticks, R, 1), wide),
            pltpu.VMEM((ticks, 2, N, R, HB), low), pltpu.VMEM((T - 1, N, R, HB), low),
            pltpu.VMEM((ticks, N, T - 1, R, PW), low), pltpu.VMEM((ticks, N - 1, T - 1, R, PW), low),
            pltpu.VMEM((ticks, T - 1, R, PW), low), pltpu.VMEM((ticks, T - 1, R, PW), low),
            pltpu.VMEM((ticks, TOK, PW), low),
            pltpu.VMEM((ticks, TOK, PW), low), pltpu.VMEM((ticks, N, T, R, PW), low),
            pltpu.VMEM((ticks, N - 1, T, R, BW), low), pltpu.VMEM((ticks, N - 1, T - 1, R, BW), low),
            pltpu.VMEM((ticks, N - 1, R, BW), low), pltpu.VMEM((ticks, N - 1, R, BW), low), pltpu.VMEM((ticks, R, BW), wide),
            pltpu.VMEM((N, R, BW), wide),
            pltpu.VMEM((BW, PW), wide), pltpu.VMEM((T - 1, BW, PW), low), pltpu.VMEM((T - 1, BW, PW), low),
            pltpu.VMEM((R, D), low), pltpu.VMEM((R, D), low), pltpu.VMEM((R, D), low), pltpu.VMEM(q.shape, low),
            pltpu.VMEM((BW, 2, PW // 2), low),
            pltpu.VMEM((ticks, 2, TOK * q.shape[-1] // (PW // 2), PW // 2), low),
            pltpu.VMEM((ticks, TOK * q.shape[-1] // (PW // 2), TOK), low),
            dma((6,)), dma((N,)), dma((T - 1,)), dma((T - 1,)),
            dma((ticks, 2, N - 1)), dma((ticks, 2, N - 1)), dma((T - 1, 2)), dma((T - 1, 2)),
            dma((ticks, N - 1)), dma((ticks, N - 1)), dma((ticks, T - 1)), dma((ticks, T - 1)),
            dma((ticks, T - 1)), dma((ticks, T - 1)), dma((4, N - 1)), dma((4, N - 1)),
            dma((ticks, N - 1, T - 1)), dma((ticks, N - 1, T - 1)), dma((ticks, N - 1)), dma((ticks, N - 1)),
            dma((T - 1, 2)), dma((T - 1, 2)), dma((1,)), dma((1,)),
        ],
        compiler_params=pltpu.CompilerParams(
            collective_id=0, has_side_effects=True, vmem_limit_bytes=62_000_000
        ),
    )(
        x, norm_gain, projection.reshape(D, 2, PW // 2), q, og, section_cotangent[0, 0], loss_cotangent[0],
        lengths.reshape(ticks), segments[0, 0],
    )
    query_grad, residual_grad, projection_grad = settle(outs)
    return (
        query_grad[None, None, :, :, None, :],
        residual_grad[None, None],
        projection_grad.reshape(1, BW, 1, 2, PW // 2),
    )


def solution(mesh):
    in_specs = (
        P("section", "dp", None, "tensor", None),
        P("section", None),
        P("section", None, "tensor", None, None),
        P("section", "dp", None, None, "tensor", None),
        P("section", "dp", None, None, "tensor", None),
        P("section", "dp", "tensor", None),
        P("dp", "tensor", None),
        P("section", "dp", None),
        P("section", "dp", None, None),
    )
    out_specs = (
        P("section", "dp", None, None, "tensor", None),
        P("section", "dp", "tensor", None),
        P("section", "dp", "tensor", None, None),
    )
    return jax.shard_map(on_device, mesh=mesh, in_specs=in_specs, out_specs=out_specs, check_vma=False)
```

```python
import functools

import jax
import jax.numpy as jnp
from jax import lax
from jax.experimental import pallas as pl
from jax.experimental.pallas import tpu as pltpu
from jax.sharding import PartitionSpec as P

EPSILON = 1e-05
MASKED = -1e30
ROWS = 16
Q = 4
FIRST = 1
NT = (((1,), (1,)), ((), ()))
TN = (((0,), (0,)), ((), ()))


def dot(left, right, dims=(((1,), (0,)), ((), ()))):
    return lax.dot_general(left, right, dims, preferred_element_type=jnp.float32)


def kernel(
    sizes,
    x_hbm, gain_ref, w_hbm, q_hbm, og_hbm, sc_hbm, lc_hbm, len_ref, seg_ref,
    qg_hbm, rg_hbm, pg_hbm,
    x, raw, w, q, og, sc, lc, wo, nb, inv, cols, rows_in, part_out, part_in, part_sum, part_all, proj,
    pair, pairs_in, back_out, back_in, feat_out, feat_in, feat_own, total,
    sum_own, sum_out, sum_in, outgoing, incoming, result, qg, pg, stacked, score_grads,
    local_sem, raw_sem, wo_s, wo_r, col_s, col_r, row_s, row_r, part_s, part_r, psum_s, psum_r,
    pair_s, pair_r, pair_fs, pair_fr, back_s, back_r, feat_s, feat_r, sum_s, sum_r, out_s, out_r,
):
    S, T, N, R, D, PW, G = sizes
    HS = PW // 2
    TOK, BW = R * T, D // N
    HB = BW // Q
    WR = min(BW, 256)
    section, me_t, me_n = (lax.axis_index(name) for name in ("section", "tensor", "dp"))
    scaling = HS ** (-0.5)

    paired = N & (N - 1) == 0

    def block_at(j):
        if not paired:
            return lax.rem(me_n + j, N)
        at = me_n
        for bit in range(j.bit_length()):
            if j >> bit & 1:
                at = at + (1 << bit) * (1 - 2 * lax.rem(lax.div(me_n, 1 << bit), 2))
        return at

    def peer(k, j):
        return {"tensor": lax.rem(me_t + k, T), "dp": block_at(j)}

    def reverse(j):
        return j if paired else (N - j) % N

    def remote(source, target, send, receive, device):
        return pltpu.make_async_remote_copy(
            src_ref=source, dst_ref=target, send_sem=send, recv_sem=receive,
            device_id=device, device_id_type=pl.DeviceIdType.MESH,
        )

    started = []

    def start(copies):
        for copy in copies:
            copy.start()
        started.extend(copies)
        return copies

    def arrive(copies):
        for copy in copies:
            copy.wait_recv()

    own_rows = pl.ds(pl.multiple_of(me_n * BW, BW), BW)

    def weight_rows(j):
        return pl.ds(pl.multiple_of(block_at(j) * BW, BW), BW)

    raw_loads = [
        pltpu.make_async_copy(w_hbm.at[weight_rows(j)], raw.at[weight_rows(j)], raw_sem.at[j]) for j in range(N)
    ]
    pairs_of = [(x_hbm.at[0], x.at[0]), (x_hbm.at[1], x.at[1]), (q_hbm, q), (og_hbm, og), (sc_hbm, sc), (lc_hbm, lc)]
    loads = [pltpu.make_async_copy(a, b, local_sem.at[i]) for i, (a, b) in enumerate(pairs_of)]
    for load in loads[:1] + raw_loads[:1] + loads[1:2] + raw_loads[1:] + loads[2:]:
        load.start()

    barrier = pltpu.get_barrier_semaphore()
    greet = [peer(k, 0) for k in range(1, T)] + [peer(0, j) for j in range(1, N)]
    down = {"section": lax.rem(section + S - 1, S)}
    greet = greet + [down, {"section": lax.rem(section + 1, S)}]
    for device in greet:
        pl.semaphore_signal(barrier, 1, device_id=device, device_id_type=pl.DeviceIdType.MESH)

    def place_weights(j):
        raw_loads[j].wait()
        first = block_at(j) * BW

        def step(i, _):
            rows = pl.ds(pl.multiple_of(first + i * WR, WR), WR)
            w[rows, :] = raw[rows].reshape(WR, PW)
            return _
        lax.fori_loop(0, BW // WR, step, 0)

    def normalize(tick):
        def step(i, _):
            rows = pl.ds(pl.multiple_of(i * ROWS, ROWS), ROWS)
            squares = jnp.zeros((ROWS, HB), jnp.float32)
            for p in range(Q * N):
                wide = x[tick, rows, p * HB:(p + 1) * HB].astype(jnp.float32)
                squares = squares + wide * wide
            inverse = lax.rsqrt(jnp.sum(squares, axis=1, keepdims=True) / D + EPSILON)
            inv[tick, rows, :] = inverse
            for p in range(Q * N):
                here = slice(p * HB, (p + 1) * HB)
                wide = x[tick, rows, here].astype(jnp.float32)
                gain = gain_ref[:, here].astype(jnp.float32)
                nb[tick, p // Q, p % Q, rows, :] = (wide * inverse * gain).astype(jnp.bfloat16)
            return _
        lax.fori_loop(0, R // ROWS, step, 0)
        cols[tick, :, 0] = nb[tick, me_n]

    def send_columns(tick, group, offsets=range(1, N)):
        pieces = [pl.ds(0, FIRST), pl.ds(FIRST, Q - FIRST)][group]
        return start([
            remote(nb.at[tick, block_at(j), pieces], cols.at[tick, pieces, j],
                   col_s.at[tick, group, j - 1], col_r.at[tick, group, j - 1], peer(0, j))
            for j in offsets
        ])

    own_tokens = pl.ds(pl.multiple_of(me_t * R, R), R)

    def tokens_of(k):
        return pl.ds(pl.multiple_of(lax.rem(me_t + k, T) * R, R), R)

    def project_own(tick):
        value = jnp.zeros((R, PW), jnp.float32)
        for p in range(Q * N):
            value = value + dot(nb[tick, p // Q, p % Q], w[p * HB:(p + 1) * HB, :])
        proj[tick, own_tokens, :] = value.astype(jnp.bfloat16)

    def send_partials(tick, halves):
        for k in range(1, T):
            value = sum(
                dot(cols[tick, h].reshape(N * R, HB), wo[k - 1, h * HB:(h + 1) * HB, :]) for h in halves
            )
            part_out[tick, :, k - 1] = value.astype(jnp.bfloat16).reshape(N, R, PW)
        return start([
            remote(part_out.at[tick, j], part_in.at[tick, j - 1],
                   part_s.at[tick, j - 1], part_r.at[tick, j - 1], peer(0, reverse(j)))
            for j in range(1, N)
        ])

    def send_part_sums(tick):
        value = part_out[tick, 0].astype(jnp.float32)
        for j in range(1, N):
            value = value + part_in[tick, j - 1].astype(jnp.float32)
        part_sum[tick] = value.astype(jnp.bfloat16)
        return start([
            remote(part_sum.at[tick, k - 1], part_all.at[tick, k - 1],
                   psum_s.at[tick, k - 1], psum_r.at[tick, k - 1], peer(T - k, 0))
            for k in range(1, T)
        ])

    def send_rows(piece):
        blocks = pl.ds(piece * (N // 2), N // 2)
        return start([
            remote(nb.at[1, blocks, pl.ds(FIRST, Q - FIRST)], rows_in.at[k - 1, blocks], row_s.at[k - 1, piece], row_r.at[k - 1, piece], peer(k, 0))
            for k in range(1, T)
        ])

    def gather_projected(tick, cross):
        for k in range(1, T):
            value = part_all[tick, k - 1].astype(jnp.float32)
            if cross:
                for p in range(N * Q):
                    if p % Q >= FIRST:
                        value = value + dot(rows_in[T - k - 1, p // Q, p % Q - FIRST], w[p * HB:(p + 1) * HB, :])
            proj[tick, tokens_of(k), :] = value.astype(jnp.bfloat16)

    position_q = lax.broadcasted_iota(jnp.int32, (TOK, TOK), 0)
    position_k = lax.broadcasted_iota(jnp.int32, (TOK, TOK), 1)

    def stack_heads(tick):
        live = lax.broadcasted_iota(jnp.int32, (TOK, HS), 0) < len_ref[tick]
        for g in range(G):
            rows, head = slice(g * TOK, (g + 1) * TOK), slice(g * HS, (g + 1) * HS)
            stacked[tick, 0, rows, :] = q[tick, :, head]
            stacked[tick, 1, rows, :] = jnp.where(live, og[tick, :, head], jnp.zeros((), jnp.bfloat16))

    def attend(tick):
        segment = jnp.broadcast_to(seg_ref[tick:tick + 1, :].astype(jnp.float32), (TOK, TOK))
        visible = (position_k <= position_q) & (segment == segment.T)
        keys, values = proj[tick, :, :HS], proj[tick, :, HS:]
        query, masked = stacked[tick, 0], stacked[tick, 1]
        scores = (dot(query, keys, NT) * scaling).reshape(G, TOK, TOK)
        scores = jnp.where(visible[None], scores, MASKED)
        weight_grad = dot(masked, values, NT).reshape(G, TOK, TOK)
        exponent = jnp.exp(scores - jnp.max(scores, axis=2, keepdims=True))
        attention = exponent * (1.0 / jnp.sum(exponent, axis=2, keepdims=True))
        low = attention.astype(jnp.bfloat16).reshape(G * TOK, TOK)
        mixed = dot(low, values)
        correction = jnp.sum(mixed * masked.astype(jnp.float32), axis=1, keepdims=True).reshape(G, TOK, 1)
        score_grad = (attention * (weight_grad - correction)).astype(jnp.bfloat16).reshape(G * TOK, TOK)
        pair[tick, :, HS:] = dot(low, masked, TN).astype(jnp.bfloat16)
        pair[tick, :, :HS] = (dot(score_grad, query, TN) * scaling).astype(jnp.bfloat16)
        score_grads[tick] = score_grad

    def finish_queries(tick):
        value = (dot(score_grads[tick], proj[tick, :, :HS]) * scaling).astype(jnp.bfloat16)
        for g in range(G):
            qg[tick, :, g * HS:(g + 1) * HS] = value[g * TOK:(g + 1) * TOK]

    def send_pairs(tick):
        pairs_in[tick, 0, 0] = pair[tick, own_tokens, :]
        return start([
            remote(pair.at[tick, tokens_of(k)], pairs_in.at[tick, 0, k],
                   pair_s.at[tick, k - 1], pair_r.at[tick, k - 1], peer(k, 0))
            for k in range(1, T)
        ])

    def forward_pairs(ticks, heads, slot, offsets=range(1, N)):
        return {
            j: start([
                remote(pairs_in.at[ticks, 0, heads], pairs_in.at[ticks, j, heads],
                       pair_fs.at[slot, j - 1], pair_fr.at[slot, j - 1], peer(0, j))
            ])
            for j in offsets
        }

    def pairs_of_head(tick, k):
        return pairs_in[tick, :, k].reshape(N * R, PW)

    def weights_of(k, columns):
        return w[pl.ds(pl.multiple_of(me_n * BW + columns.start, CH), columns.stop - columns.start), :] \
            if k == 0 else wo[k - 1, columns, :]

    CH = min(BW, 512)

    def send_back(tick, j):
        b = block_at(j)
        for c in range(0, BW, CH):
            rows = pl.ds(pl.multiple_of(b * BW + c, CH), CH)
            value = dot(pair[tick], w[rows, :], NT).astype(jnp.bfloat16)
            back_out[tick, j - 1, :, :, c:c + CH] = value.reshape(T, R, CH)
        return start([
            remote(back_out.at[tick, j - 1, lax.rem(me_t + k, T)], back_in.at[tick, j - 1, k - 1],
                   back_s.at[tick, j - 1, k - 1], back_r.at[tick, j - 1, k - 1], peer(k, 0))
            for k in range(1, T)
        ])

    def feature_grads(tick, slots):
        for c in range(0, BW, CH):
            here = slice(c, c + CH)
            value = jnp.zeros((slots * R, CH), jnp.float32)
            for k in range(T):
                pairs = pairs_in[tick, :slots, k].reshape(slots * R, PW)
                term = dot(pairs, weights_of(k, here), NT)
                value = value + term.astype(jnp.bfloat16).astype(jnp.float32)
            feat_own[tick, :, here] = value[:R]
            feat_out[tick, :slots - 1, :, here] = value[R:].astype(jnp.bfloat16).reshape(slots - 1, R, CH)

    def send_features(tick, offsets):
        return {
            j: start([
                remote(feat_out.at[tick, j - 1], feat_in.at[tick, j - 1],
                       feat_s.at[tick, j - 1], feat_r.at[tick, j - 1], peer(0, reverse(j)))
            ])
            for j in offsets
        }

    def collect(tick, backs, features):
        total[me_n] = feat_own[tick]
        for j in backs:
            arrive(backs[j])
            value = back_out[tick, j - 1, me_t].astype(jnp.float32)
            for k in range(1, T):
                value = value + back_in[tick, j - 1, k - 1].astype(jnp.float32)
            total[block_at(j)] = value
        for j in features:
            arrive(features[j])
            total[block_at(j)] = feat_in[tick, j - 1].astype(jnp.float32)

    def norm_back(tick, base, target):
        def step(i, _):
            rows = pl.ds(pl.multiple_of(i * ROWS, ROWS), ROWS)
            inverse = inv[tick, rows, :]
            products = jnp.zeros((ROWS, BW), jnp.float32)
            for b in range(N):
                here = slice(b * BW, (b + 1) * BW)
                scaled = total[b, rows, :] * gain_ref[:, here].astype(jnp.float32)
                products = products + scaled * x[tick, rows, here].astype(jnp.float32)
            mean = jnp.sum(products, axis=1, keepdims=True) / D
            cube = inverse * inverse * inverse * mean
            for b in range(N):
                here = slice(b * BW, (b + 1) * BW)
                scaled = total[b, rows, :] * gain_ref[:, here].astype(jnp.float32)
                back = inverse * scaled - x[tick, rows, here].astype(jnp.float32) * cube
                target[rows, here] = (base(rows, here) + back).astype(jnp.bfloat16)
            return _
        lax.fori_loop(0, R // ROWS, step, 0)

    def accumulate(k, h):
        here = slice(h * HB, (h + 1) * HB)
        value = sum(dot(cols[tick, h].reshape(N * R, HB), pairs_of_head(tick, k), TN) for tick in range(2))
        if k == 0:
            sum_own[here, :] = value
        else:
            sum_out[k - 1, here, :] = value.astype(jnp.bfloat16)

    by_tensor = [list(range(2, N)), [N // 2]]
    by_dp = [[j for j in range(1, N) if j not in by_tensor[tick]] for tick in range(2)]

    loads[0].wait()
    normalize(0)
    pl.semaphore_wait(barrier, len(greet))
    columns_sent = {(0, h): send_columns(0, h) for h in range(2)}
    place_weights(0)
    weights_sent = start([
        remote(w.at[own_rows], wo.at[k - 1], wo_s.at[k - 1], wo_r.at[k - 1], peer(k, 0)) for k in range(1, T)
    ])
    loads[1].wait()
    normalize(1)
    rows_sent = send_rows(0)
    for j in range(1, N):
        place_weights(j)
    for tick in range(2):
        project_own(tick)
    for load in loads[2:4]:
        load.wait()
    for tick in range(2):
        stack_heads(tick)

    arrive(weights_sent)
    for group in range(2):
        arrive(columns_sent[0, group])
    near, far = range(1, 2), range(2, N)
    partials = send_partials(0, range(Q))
    columns_sent[1, 0] = send_columns(1, 0, near)
    columns_sent[1, 0] = columns_sent[1, 0] + send_columns(1, 0, far)
    arrive(partials)
    part_sums = [send_part_sums(0)]
    rows_sent = rows_sent + send_rows(1)
    arrive(part_sums[0])
    gather_projected(0, False)
    attend(0)
    pairs_sent = send_pairs(0)
    backs = [{}, {}]
    first, *rest = by_tensor[0]
    backs[0][first] = send_back(0, first)
    arrive(columns_sent[1, 0])
    partials = send_partials(1, range(FIRST))
    columns_sent[1, 1] = send_columns(1, 1, near)
    columns_sent[1, 1] = columns_sent[1, 1] + send_columns(1, 1, far)
    finish_queries(0)
    arrive(partials)
    part_sums.append(send_part_sums(1))
    arrive(pairs_sent)
    everyone, others, own_head = pl.ds(0, T), pl.ds(1, T - 1), pl.ds(0, 1)
    near_moved = forward_pairs(pl.ds(0, 1), everyone, 0, near)
    others_moved = [forward_pairs(pl.ds(0, 1), others, 0, far)]
    for j in rest:
        backs[0][j] = send_back(0, j)
    arrive(rows_sent)
    arrive(part_sums[1])
    gather_projected(1, True)
    attend(1)
    pairs_sent = send_pairs(1)
    arrive(pairs_sent)
    others_moved.append(forward_pairs(pl.ds(1, 1), others, 1))
    arrive(near_moved[1])
    feature_grads(0, 2)
    features = [send_features(0, near)]
    late_moved = [forward_pairs(pl.ds(1, 1), own_head, 2), forward_pairs(pl.ds(0, 1), own_head, 3, far)]
    for j in by_tensor[1]:
        backs[1][j] = send_back(1, j)
    finish_queries(1)
    query_out = pltpu.make_async_copy(qg, qg_hbm, local_sem.at[2])
    query_out.start()

    for moved in others_moved:
        for j in moved:
            arrive(moved[j])
    arrive(columns_sent[1, 1])
    sums_sent = []
    for k in range(1, T):
        for h in range(Q):
            here = pl.ds(h * HB, HB)
            accumulate(k, h)
            sums_sent += start([
                remote(sum_out.at[k - 1, here], sum_in.at[k - 1, here],
                       sum_s.at[k - 1, h], sum_r.at[k - 1, h], peer(T - k, 0))
            ])

    collect(0, backs[0], features[0])
    loads[4].wait()
    loads[5].wait()
    norm_back(0, lambda rows, here: sc[rows, here].astype(jnp.float32), outgoing)
    shift = start([remote(outgoing, incoming, out_s.at[0], out_r.at[0], down)])
    for moved in late_moved:
        for j in moved:
            arrive(moved[j])
    feature_grads(1, N)
    features.append(send_features(1, by_dp[1]))
    for h in range(Q):
        accumulate(0, h)

    collect(1, backs[1], features[1])
    arrive(shift)
    is_last = section == S - 1

    def arriving(rows, here):
        return jnp.where(is_last, lc[rows, here].astype(jnp.float32), incoming[rows, here].astype(jnp.float32))

    norm_back(1, arriving, result)
    residual_out = pltpu.make_async_copy(result, rg_hbm, local_sem.at[0])
    residual_out.start()

    arrive(sums_sent)

    def finish(i, _):
        rows = pl.ds(pl.multiple_of(i * WR, WR), WR)
        final = sum_own[rows, :]
        for k in range(1, T):
            final = final + sum_in[k - 1, rows, :].astype(jnp.float32)
        pg[rows] = final.astype(jnp.bfloat16).reshape(WR, 2, HS)
        return _

    lax.fori_loop(0, BW // WR, finish, 0)
    weight_out = pltpu.make_async_copy(pg, pg_hbm, local_sem.at[1])
    weight_out.start()
    for copy in started:
        copy.wait_send()
    query_out.wait()
    residual_out.wait()
    weight_out.wait()


def copies(*refs):
    count = (len(refs) - 1) // 3
    sources, targets, held, sems = refs[:count], refs[count:2 * count], refs[2 * count:3 * count], refs[-1]
    moves = [
        [pltpu.make_async_copy(source, buffer, sems.at[i, 0]), pltpu.make_async_copy(buffer, target, sems.at[i, 1])]
        for i, (source, target, buffer) in enumerate(zip(sources, targets, held))
    ]
    for inward, _ in moves:
        inward.start()
    for inward, outward in moves:
        inward.wait()
        outward.start()
    for _, outward in moves:
        outward.wait()


def settle(arrays):
    anywhere = pl.BlockSpec(memory_space=pl.ANY)
    return pl.pallas_call(
        copies,
        out_shape=tuple(jax.ShapeDtypeStruct(array.shape, array.dtype) for array in arrays),
        in_specs=[anywhere] * len(arrays),
        out_specs=[anywhere] * len(arrays),
        scratch_shapes=[pltpu.VMEM(array.shape, array.dtype) for array in arrays] + [pltpu.SemaphoreType.DMA((len(arrays), 2))],
    )(*arrays)


def on_device(residuals, norm_gain, projection, queries, output_grad, section_cotangent, loss_cotangent, lengths, segments):
    x, q, og = residuals[0, 0], queries[0, 0, :, :, 0, :], output_grad[0, 0, :, :, 0, :]
    ticks, R, D = x.shape
    PW = 2 * projection.shape[4]
    S, T, N = (lax.axis_size(name) for name in ("section", "tensor", "dp"))
    TOK, BW, HB = R * T, D // N, D // N // Q
    sizes = (S, T, N, R, D, PW, q.shape[-1] // (PW // 2))
    low, wide, dma = jnp.bfloat16, jnp.float32, pltpu.SemaphoreType.DMA
    anywhere, vmem = pl.BlockSpec(memory_space=pl.ANY), pl.BlockSpec(memory_space=pltpu.VMEM)
    outs = pl.pallas_call(
        functools.partial(kernel, sizes),
        out_shape=(
            jax.ShapeDtypeStruct(q.shape, low),
            jax.ShapeDtypeStruct((R, D), low),
            jax.ShapeDtypeStruct((BW, 2, PW // 2), low),
        ),
        in_specs=[anywhere, vmem] + [anywhere] * 5 + [pl.BlockSpec(memory_space=pltpu.SMEM), vmem],
        out_specs=[anywhere] * 3,
        scratch_shapes=[
            pltpu.VMEM(x.shape, low), pltpu.VMEM((D, 2, PW // 2), low), pltpu.VMEM((D, PW), low), pltpu.VMEM(q.shape, low), pltpu.VMEM(q.shape, low),
            pltpu.VMEM((R, D), low), pltpu.VMEM((R, D), low),
            pltpu.VMEM((T - 1, BW, PW), low),
            pltpu.VMEM((ticks, N, Q, R, HB), low), pltpu.VMEM((ticks, R, 1), wide),
            pltpu.VMEM((ticks, Q, N, R, HB), low), pltpu.VMEM((T - 1, N, Q - FIRST, R, HB), low),
            pltpu.VMEM((ticks, N, T - 1, R, PW), low), pltpu.VMEM((ticks, N - 1, T - 1, R, PW), low),
            pltpu.VMEM((ticks, T - 1, R, PW), low), pltpu.VMEM((ticks, T - 1, R, PW), low),
            pltpu.VMEM((ticks, TOK, PW), low),
            pltpu.VMEM((ticks, TOK, PW), low), pltpu.VMEM((ticks, N, T, R, PW), low),
            pltpu.VMEM((ticks, N - 1, T, R, BW), low), pltpu.VMEM((ticks, N - 1, T - 1, R, BW), low),
            pltpu.VMEM((ticks, N - 1, R, BW), low), pltpu.VMEM((ticks, N - 1, R, BW), low), pltpu.VMEM((ticks, R, BW), wide),
            pltpu.VMEM((N, R, BW), wide),
            pltpu.VMEM((BW, PW), wide), pltpu.VMEM((T - 1, BW, PW), low), pltpu.VMEM((T - 1, BW, PW), low),
            pltpu.VMEM((R, D), low), pltpu.VMEM((R, D), low), pltpu.VMEM((R, D), low), pltpu.VMEM(q.shape, low),
            pltpu.VMEM((BW, 2, PW // 2), low),
            pltpu.VMEM((ticks, 2, TOK * q.shape[-1] // (PW // 2), PW // 2), low),
            pltpu.VMEM((ticks, TOK * q.shape[-1] // (PW // 2), TOK), low),
            dma((6,)), dma((N,)), dma((T - 1,)), dma((T - 1,)),
            dma((ticks, 2, N - 1)), dma((ticks, 2, N - 1)), dma((T - 1, 2)), dma((T - 1, 2)),
            dma((ticks, N - 1)), dma((ticks, N - 1)), dma((ticks, T - 1)), dma((ticks, T - 1)),
            dma((ticks, T - 1)), dma((ticks, T - 1)), dma((4, N - 1)), dma((4, N - 1)),
            dma((ticks, N - 1, T - 1)), dma((ticks, N - 1, T - 1)), dma((ticks, N - 1)), dma((ticks, N - 1)),
            dma((T - 1, Q)), dma((T - 1, Q)), dma((1,)), dma((1,)),
        ],
        compiler_params=pltpu.CompilerParams(
            collective_id=0, has_side_effects=True, vmem_limit_bytes=62_000_000
        ),
    )(
        x, norm_gain, projection.reshape(D, 2, PW // 2), q, og, section_cotangent[0, 0], loss_cotangent[0],
        lengths.reshape(ticks), segments[0, 0],
    )
    query_grad, residual_grad, projection_grad = settle(outs)
    return (
        query_grad[None, None, :, :, None, :],
        residual_grad[None, None],
        projection_grad.reshape(1, BW, 1, 2, PW // 2),
    )


def solution(mesh):
    in_specs = (
        P("section", "dp", None, "tensor", None),
        P("section", None),
        P("section", None, "tensor", None, None),
        P("section", "dp", None, None, "tensor", None),
        P("section", "dp", None, None, "tensor", None),
        P("section", "dp", "tensor", None),
        P("dp", "tensor", None),
        P("section", "dp", None),
        P("section", "dp", None, None),
    )
    out_specs = (
        P("section", "dp", None, None, "tensor", None),
        P("section", "dp", "tensor", None),
        P("section", "dp", "tensor", None, None),
    )
    return jax.shard_map(on_device, mesh=mesh, in_specs=in_specs, out_specs=out_specs, check_vma=False)
```

```python
import functools

import jax
import jax.numpy as jnp
from jax import lax
from jax.experimental import pallas as pl
from jax.experimental.pallas import tpu as pltpu
from jax.sharding import PartitionSpec as P

EPSILON = 1e-05
MASKED = -1e30
ROWS = 16
Q = 4
FIRST = 1
NT = (((1,), (1,)), ((), ()))
TN = (((0,), (0,)), ((), ()))


def dot(left, right, dims=(((1,), (0,)), ((), ()))):
    return lax.dot_general(left, right, dims, preferred_element_type=jnp.float32)


def kernel(
    sizes,
    x_hbm, gain_ref, w_hbm, q_hbm, og_hbm, sc_hbm, lc_hbm, len_ref, seg_ref,
    qg_hbm, rg_hbm, pg_hbm,
    x, raw, w, q, og, sc, lc, wo, nb, inv, cols, rows_in, part_out, part_in, part_sum, part_all, proj,
    pair, pairs_in, back_out, back_in, feat_out, feat_in, feat_own, total,
    sum_own, sum_out, sum_in, outgoing, incoming, result, qg, pg, stacked, score_grads,
    local_sem, raw_sem, wo_s, wo_r, col_s, col_r, row_s, row_r, part_s, part_r, psum_s, psum_r,
    pair_s, pair_r, pair_fs, pair_fr, back_s, back_r, feat_s, feat_r, sum_s, sum_r, out_s, out_r,
):
    S, T, N, R, D, PW, G = sizes
    HS = PW // 2
    TOK, BW = R * T, D // N
    HB = BW // Q
    WR = min(BW, 256)
    section, me_t, me_n = (lax.axis_index(name) for name in ("section", "tensor", "dp"))
    scaling = HS ** (-0.5)

    paired = N & (N - 1) == 0

    def block_at(j):
        if not paired:
            return lax.rem(me_n + j, N)
        at = me_n
        for bit in range(j.bit_length()):
            if j >> bit & 1:
                at = at + (1 << bit) * (1 - 2 * lax.rem(lax.div(me_n, 1 << bit), 2))
        return at

    def peer(k, j):
        return {"tensor": lax.rem(me_t + k, T), "dp": block_at(j)}

    def reverse(j):
        return j if paired else (N - j) % N

    def remote(source, target, send, receive, device):
        return pltpu.make_async_remote_copy(
            src_ref=source, dst_ref=target, send_sem=send, recv_sem=receive,
            device_id=device, device_id_type=pl.DeviceIdType.MESH,
        )

    started = []

    def start(copies):
        for copy in copies:
            copy.start()
        started.extend(copies)
        return copies

    def arrive(copies):
        for copy in copies:
            copy.wait_recv()

    def weight_rows(j):
        return pl.ds(pl.multiple_of(block_at(j) * BW, BW), BW)

    raw_loads = [
        pltpu.make_async_copy(w_hbm.at[weight_rows(j)], raw.at[weight_rows(j)], raw_sem.at[j]) for j in range(N)
    ]
    pairs_of = [(x_hbm.at[0], x.at[0]), (x_hbm.at[1], x.at[1]), (q_hbm, q), (og_hbm, og), (sc_hbm, sc), (lc_hbm, lc)]
    loads = [pltpu.make_async_copy(a, b, local_sem.at[i]) for i, (a, b) in enumerate(pairs_of)]
    for load in loads[:1] + raw_loads[:1] + loads[1:2] + raw_loads[1:] + loads[2:]:
        load.start()

    barrier = pltpu.get_barrier_semaphore()
    greet = [peer(k, 0) for k in range(1, T)] + [peer(0, j) for j in range(1, N)]
    down = {"section": lax.rem(section + S - 1, S)}
    greet = greet + [down, {"section": lax.rem(section + 1, S)}]
    for device in greet:
        pl.semaphore_signal(barrier, 1, device_id=device, device_id_type=pl.DeviceIdType.MESH)

    def place_weights(j, part=0, parts=1):
        if part == 0:
            raw_loads[j].wait()
        first = block_at(j) * BW + part * (BW // parts)

        def step(i, _):
            rows = pl.ds(pl.multiple_of(first + i * WR, WR), WR)
            w[rows, :] = raw[rows].reshape(WR, PW)
            return _
        lax.fori_loop(0, BW // parts // WR, step, 0)

    def normalize(tick):
        def step(i, _):
            rows = pl.ds(pl.multiple_of(i * ROWS, ROWS), ROWS)
            squares = jnp.zeros((ROWS, HB), jnp.float32)
            for p in range(Q * N):
                wide = x[tick, rows, p * HB:(p + 1) * HB].astype(jnp.float32)
                squares = squares + wide * wide
            inverse = lax.rsqrt(jnp.sum(squares, axis=1, keepdims=True) / D + EPSILON)
            inv[tick, rows, :] = inverse
            for p in range(Q * N):
                here = slice(p * HB, (p + 1) * HB)
                wide = x[tick, rows, here].astype(jnp.float32)
                gain = gain_ref[:, here].astype(jnp.float32)
                nb[tick, p // Q, p % Q, rows, :] = (wide * inverse * gain).astype(jnp.bfloat16)
            return _
        lax.fori_loop(0, R // ROWS, step, 0)
        cols[tick, :, 0] = nb[tick, me_n]

    def send_columns(tick, group, offsets=range(1, N)):
        pieces = [pl.ds(0, FIRST), pl.ds(FIRST, Q - FIRST)][group]
        return start([
            remote(nb.at[tick, block_at(j), pieces], cols.at[tick, pieces, j],
                   col_s.at[tick, group, j - 1], col_r.at[tick, group, j - 1], peer(0, j))
            for j in offsets
        ])

    own_tokens = pl.ds(pl.multiple_of(me_t * R, R), R)

    def tokens_of(k):
        return pl.ds(pl.multiple_of(lax.rem(me_t + k, T) * R, R), R)

    def project_own(tick):
        value = jnp.zeros((R, PW), jnp.float32)
        for p in range(Q * N):
            value = value + dot(nb[tick, p // Q, p % Q], w[p * HB:(p + 1) * HB, :])
        proj[tick, own_tokens, :] = value.astype(jnp.bfloat16)

    def send_partials(tick, halves):
        for k in range(1, T):
            value = sum(
                dot(cols[tick, h].reshape(N * R, HB), wo[k - 1, h * HB:(h + 1) * HB, :]) for h in halves
            )
            part_out[tick, :, k - 1] = value.astype(jnp.bfloat16).reshape(N, R, PW)
        return start([
            remote(part_out.at[tick, j], part_in.at[tick, j - 1],
                   part_s.at[tick, j - 1], part_r.at[tick, j - 1], peer(0, reverse(j)))
            for j in range(1, N)
        ])

    def send_part_sums(tick):
        value = part_out[tick, 0].astype(jnp.float32)
        for j in range(1, N):
            value = value + part_in[tick, j - 1].astype(jnp.float32)
        part_sum[tick] = value.astype(jnp.bfloat16)
        return start([
            remote(part_sum.at[tick, k - 1], part_all.at[tick, k - 1],
                   psum_s.at[tick, k - 1], psum_r.at[tick, k - 1], peer(T - k, 0))
            for k in range(1, T)
        ])

    def send_rows(piece):
        blocks = pl.ds(piece * (N // 2), N // 2)
        return start([
            remote(nb.at[1, blocks, pl.ds(FIRST, Q - FIRST)], rows_in.at[k - 1, blocks], row_s.at[k - 1, piece], row_r.at[k - 1, piece], peer(k, 0))
            for k in range(1, T)
        ])

    def gather_projected(tick, cross):
        for k in range(1, T):
            value = part_all[tick, k - 1].astype(jnp.float32)
            if cross:
                for p in range(N * Q):
                    if p % Q >= FIRST:
                        value = value + dot(rows_in[T - k - 1, p // Q, p % Q - FIRST], w[p * HB:(p + 1) * HB, :])
            proj[tick, tokens_of(k), :] = value.astype(jnp.bfloat16)

    position_q = lax.broadcasted_iota(jnp.int32, (TOK, TOK), 0)
    position_k = lax.broadcasted_iota(jnp.int32, (TOK, TOK), 1)

    def stack_heads(tick):
        live = lax.broadcasted_iota(jnp.int32, (TOK, HS), 0) < len_ref[tick]
        for g in range(G):
            rows, head = slice(g * TOK, (g + 1) * TOK), slice(g * HS, (g + 1) * HS)
            stacked[tick, 0, rows, :] = q[tick, :, head]
            stacked[tick, 1, rows, :] = jnp.where(live, og[tick, :, head], jnp.zeros((), jnp.bfloat16))

    def attend(tick):
        segment = jnp.broadcast_to(seg_ref[tick:tick + 1, :].astype(jnp.float32), (TOK, TOK))
        visible = (position_k <= position_q) & (segment == segment.T)
        keys, values = proj[tick, :, :HS], proj[tick, :, HS:]
        query, masked = stacked[tick, 0], stacked[tick, 1]
        scores = (dot(query, keys, NT) * scaling).reshape(G, TOK, TOK)
        scores = jnp.where(visible[None], scores, MASKED)
        weight_grad = dot(masked, values, NT).reshape(G, TOK, TOK)
        exponent = jnp.exp(scores - jnp.max(scores, axis=2, keepdims=True))
        attention = exponent * (1.0 / jnp.sum(exponent, axis=2, keepdims=True))
        low = attention.astype(jnp.bfloat16).reshape(G * TOK, TOK)
        mixed = dot(low, values)
        correction = jnp.sum(mixed * masked.astype(jnp.float32), axis=1, keepdims=True).reshape(G, TOK, 1)
        score_grad = (attention * (weight_grad - correction)).astype(jnp.bfloat16).reshape(G * TOK, TOK)
        pair[tick, :, HS:] = dot(low, masked, TN).astype(jnp.bfloat16)
        pair[tick, :, :HS] = (dot(score_grad, query, TN) * scaling).astype(jnp.bfloat16)
        score_grads[tick] = score_grad

    def finish_queries(tick):
        value = (dot(score_grads[tick], proj[tick, :, :HS]) * scaling).astype(jnp.bfloat16)
        for g in range(G):
            qg[tick, :, g * HS:(g + 1) * HS] = value[g * TOK:(g + 1) * TOK]

    def send_pairs(tick):
        pairs_in[tick, 0, 0] = pair[tick, own_tokens, :]
        return start([
            remote(pair.at[tick, tokens_of(k)], pairs_in.at[tick, 0, k],
                   pair_s.at[tick, k - 1], pair_r.at[tick, k - 1], peer(k, 0))
            for k in range(1, T)
        ])

    def forward_pairs(ticks, heads, slot, offsets=range(1, N)):
        return {
            j: start([
                remote(pairs_in.at[ticks, 0, heads], pairs_in.at[ticks, j, heads],
                       pair_fs.at[slot, j - 1], pair_fr.at[slot, j - 1], peer(0, j))
            ])
            for j in offsets
        }

    def pairs_of_head(tick, k):
        return pairs_in[tick, :, k].reshape(N * R, PW)

    def weights_of(k, columns):
        return w[pl.ds(pl.multiple_of(me_n * BW + columns.start, CH), columns.stop - columns.start), :] \
            if k == 0 else wo[k - 1, columns, :]

    CH = min(BW, 512)

    def send_back(tick, j):
        b = block_at(j)
        for c in range(0, BW, CH):
            rows = pl.ds(pl.multiple_of(b * BW + c, CH), CH)
            value = dot(pair[tick], w[rows, :], NT).astype(jnp.bfloat16)
            back_out[tick, j - 1, :, :, c:c + CH] = value.reshape(T, R, CH)
        return start([
            remote(back_out.at[tick, j - 1, lax.rem(me_t + k, T)], back_in.at[tick, j - 1, k - 1],
                   back_s.at[tick, j - 1, k - 1], back_r.at[tick, j - 1, k - 1], peer(k, 0))
            for k in range(1, T)
        ])

    def feature_grads(tick, slots):
        for c in range(0, BW, CH):
            here = slice(c, c + CH)
            value = jnp.zeros((slots * R, CH), jnp.float32)
            for k in range(T):
                pairs = pairs_in[tick, :slots, k].reshape(slots * R, PW)
                term = dot(pairs, weights_of(k, here), NT)
                value = value + term.astype(jnp.bfloat16).astype(jnp.float32)
            feat_own[tick, :, here] = value[:R]
            feat_out[tick, :slots - 1, :, here] = value[R:].astype(jnp.bfloat16).reshape(slots - 1, R, CH)

    def send_features(tick, offsets):
        return {
            j: start([
                remote(feat_out.at[tick, j - 1], feat_in.at[tick, j - 1],
                       feat_s.at[tick, j - 1], feat_r.at[tick, j - 1], peer(0, reverse(j)))
            ])
            for j in offsets
        }

    def collect(tick, backs, features):
        total[me_n] = feat_own[tick]
        for j in backs:
            arrive(backs[j])
            value = back_out[tick, j - 1, me_t].astype(jnp.float32)
            for k in range(1, T):
                value = value + back_in[tick, j - 1, k - 1].astype(jnp.float32)
            total[block_at(j)] = value
        for j in features:
            arrive(features[j])
            total[block_at(j)] = feat_in[tick, j - 1].astype(jnp.float32)

    def norm_back(tick, base, target):
        def step(i, _):
            rows = pl.ds(pl.multiple_of(i * ROWS, ROWS), ROWS)
            inverse = inv[tick, rows, :]
            products = jnp.zeros((ROWS, BW), jnp.float32)
            for b in range(N):
                here = slice(b * BW, (b + 1) * BW)
                scaled = total[b, rows, :] * gain_ref[:, here].astype(jnp.float32)
                products = products + scaled * x[tick, rows, here].astype(jnp.float32)
            mean = jnp.sum(products, axis=1, keepdims=True) / D
            cube = inverse * inverse * inverse * mean
            for b in range(N):
                here = slice(b * BW, (b + 1) * BW)
                scaled = total[b, rows, :] * gain_ref[:, here].astype(jnp.float32)
                back = inverse * scaled - x[tick, rows, here].astype(jnp.float32) * cube
                target[rows, here] = (base(rows, here) + back).astype(jnp.bfloat16)
            return _
        lax.fori_loop(0, R // ROWS, step, 0)

    def accumulate(k, h):
        here = slice(h * HB, (h + 1) * HB)
        value = sum(dot(cols[tick, h].reshape(N * R, HB), pairs_of_head(tick, k), TN) for tick in range(2))
        if k == 0:
            sum_own[here, :] = value
        else:
            sum_out[k - 1, here, :] = value.astype(jnp.bfloat16)

    by_tensor = [list(range(2, N)), [N // 2]]
    by_dp = [[j for j in range(1, N) if j not in by_tensor[tick]] for tick in range(2)]

    loads[0].wait()
    normalize(0)
    pl.semaphore_wait(barrier, len(greet))
    columns_sent = {(0, h): send_columns(0, h) for h in range(2)}
    weights_sent = []
    for part in range(2):
        place_weights(0, part, 2)
        rows = pl.ds(pl.multiple_of(me_n * BW + part * (BW // 2), BW // 2), BW // 2)
        weights_sent += start([
            remote(w.at[rows], wo.at[k - 1, pl.ds(part * (BW // 2), BW // 2)],
                   wo_s.at[k - 1, part], wo_r.at[k - 1, part], peer(k, 0))
            for k in range(1, T)
        ])
    loads[1].wait()
    normalize(1)
    rows_sent = send_rows(0)
    for j in range(1, N):
        place_weights(j)
    for tick in range(2):
        project_own(tick)
    for load in loads[2:4]:
        load.wait()
    for tick in range(2):
        stack_heads(tick)

    arrive(weights_sent)
    for group in range(2):
        arrive(columns_sent[0, group])
    near, far = range(1, 2), range(2, N)
    partials = send_partials(0, range(Q))
    columns_sent[1, 0] = send_columns(1, 0, near)
    columns_sent[1, 0] = columns_sent[1, 0] + send_columns(1, 0, far)
    arrive(partials)
    part_sums = [send_part_sums(0)]
    rows_sent = rows_sent + send_rows(1)
    arrive(part_sums[0])
    gather_projected(0, False)
    attend(0)
    pairs_sent = send_pairs(0)
    backs = [{}, {}]
    first, *rest = by_tensor[0]
    backs[0][first] = send_back(0, first)
    arrive(columns_sent[1, 0])
    partials = send_partials(1, range(FIRST))
    columns_sent[1, 1] = send_columns(1, 1, near)
    columns_sent[1, 1] = columns_sent[1, 1] + send_columns(1, 1, far)
    finish_queries(0)
    arrive(partials)
    part_sums.append(send_part_sums(1))
    arrive(pairs_sent)
    everyone, others, own_head = pl.ds(0, T), pl.ds(1, T - 1), pl.ds(0, 1)
    near_moved = forward_pairs(pl.ds(0, 1), everyone, 0, near)
    others_moved = [forward_pairs(pl.ds(0, 1), others, 0, far)]
    for j in rest:
        backs[0][j] = send_back(0, j)
    arrive(rows_sent)
    arrive(part_sums[1])
    gather_projected(1, True)
    attend(1)
    pairs_sent = send_pairs(1)
    arrive(pairs_sent)
    others_moved.append(forward_pairs(pl.ds(1, 1), others, 1))
    arrive(near_moved[1])
    feature_grads(0, 2)
    features = [send_features(0, near)]
    late_moved = [forward_pairs(pl.ds(1, 1), own_head, 2), forward_pairs(pl.ds(0, 1), own_head, 3, far)]
    for j in by_tensor[1]:
        backs[1][j] = send_back(1, j)
    finish_queries(1)
    query_out = pltpu.make_async_copy(qg, qg_hbm, local_sem.at[2])
    query_out.start()

    for moved in others_moved:
        for j in moved:
            arrive(moved[j])
    arrive(columns_sent[1, 1])
    sums_sent = []
    for k in range(1, T):
        for h in range(Q):
            here = pl.ds(h * HB, HB)
            accumulate(k, h)
            sums_sent += start([
                remote(sum_out.at[k - 1, here], sum_in.at[k - 1, here],
                       sum_s.at[k - 1, h], sum_r.at[k - 1, h], peer(T - k, 0))
            ])

    collect(0, backs[0], features[0])
    loads[4].wait()
    loads[5].wait()
    norm_back(0, lambda rows, here: sc[rows, here].astype(jnp.float32), outgoing)
    shift = start([remote(outgoing, incoming, out_s.at[0], out_r.at[0], down)])
    for moved in late_moved:
        for j in moved:
            arrive(moved[j])
    feature_grads(1, N)
    features.append(send_features(1, by_dp[1]))
    for h in range(Q):
        accumulate(0, h)

    collect(1, backs[1], features[1])
    arrive(shift)
    is_last = section == S - 1

    def arriving(rows, here):
        return jnp.where(is_last, lc[rows, here].astype(jnp.float32), incoming[rows, here].astype(jnp.float32))

    norm_back(1, arriving, result)
    residual_out = pltpu.make_async_copy(result, rg_hbm, local_sem.at[0])
    residual_out.start()

    arrive(sums_sent)

    def finish(i, _):
        rows = pl.ds(pl.multiple_of(i * WR, WR), WR)
        final = sum_own[rows, :]
        for k in range(1, T):
            final = final + sum_in[k - 1, rows, :].astype(jnp.float32)
        pg[rows] = final.astype(jnp.bfloat16).reshape(WR, 2, HS)
        return _

    lax.fori_loop(0, BW // WR, finish, 0)
    weight_out = pltpu.make_async_copy(pg, pg_hbm, local_sem.at[1])
    weight_out.start()
    for copy in started:
        copy.wait_send()
    query_out.wait()
    residual_out.wait()
    weight_out.wait()


def copies(*refs):
    count = (len(refs) - 1) // 3
    sources, targets, held, sems = refs[:count], refs[count:2 * count], refs[2 * count:3 * count], refs[-1]
    moves = []
    for i, (source, target, buffer) in enumerate(zip(sources, targets, held)):
        pieces = min(4, source.shape[0] // ROWS) or source.shape[0]
        size = source.shape[0] // pieces
        for p in range(pieces):
            rows = pl.ds(p * size, size)
            moves.append((
                pltpu.make_async_copy(source.at[rows], buffer.at[rows], sems.at[i, p, 0]),
                pltpu.make_async_copy(buffer.at[rows], target.at[rows], sems.at[i, p, 1]),
            ))
    for inward, _ in moves:
        inward.start()
    for inward, outward in moves:
        inward.wait()
        outward.start()
    for _, outward in moves:
        outward.wait()


def settle(arrays):
    anywhere = pl.BlockSpec(memory_space=pl.ANY)
    return pl.pallas_call(
        copies,
        out_shape=tuple(jax.ShapeDtypeStruct(array.shape, array.dtype) for array in arrays),
        in_specs=[anywhere] * len(arrays),
        out_specs=[anywhere] * len(arrays),
        scratch_shapes=[pltpu.VMEM(array.shape, array.dtype) for array in arrays]
        + [pltpu.SemaphoreType.DMA((len(arrays), 4, 2))],
    )(*arrays)


def on_device(residuals, norm_gain, projection, queries, output_grad, section_cotangent, loss_cotangent, lengths, segments):
    x, q, og = residuals[0, 0], queries[0, 0, :, :, 0, :], output_grad[0, 0, :, :, 0, :]
    ticks, R, D = x.shape
    PW = 2 * projection.shape[4]
    S, T, N = (lax.axis_size(name) for name in ("section", "tensor", "dp"))
    TOK, BW, HB = R * T, D // N, D // N // Q
    sizes = (S, T, N, R, D, PW, q.shape[-1] // (PW // 2))
    low, wide, dma = jnp.bfloat16, jnp.float32, pltpu.SemaphoreType.DMA
    anywhere, vmem = pl.BlockSpec(memory_space=pl.ANY), pl.BlockSpec(memory_space=pltpu.VMEM)
    outs = pl.pallas_call(
        functools.partial(kernel, sizes),
        out_shape=(
            jax.ShapeDtypeStruct(q.shape, low),
            jax.ShapeDtypeStruct((R, D), low),
            jax.ShapeDtypeStruct((BW, 2, PW // 2), low),
        ),
        in_specs=[anywhere, vmem] + [anywhere] * 5 + [pl.BlockSpec(memory_space=pltpu.SMEM), vmem],
        out_specs=[anywhere] * 3,
        scratch_shapes=[
            pltpu.VMEM(x.shape, low), pltpu.VMEM((D, 2, PW // 2), low), pltpu.VMEM((D, PW), low), pltpu.VMEM(q.shape, low), pltpu.VMEM(q.shape, low),
            pltpu.VMEM((R, D), low), pltpu.VMEM((R, D), low),
            pltpu.VMEM((T - 1, BW, PW), low),
            pltpu.VMEM((ticks, N, Q, R, HB), low), pltpu.VMEM((ticks, R, 1), wide),
            pltpu.VMEM((ticks, Q, N, R, HB), low), pltpu.VMEM((T - 1, N, Q - FIRST, R, HB), low),
            pltpu.VMEM((ticks, N, T - 1, R, PW), low), pltpu.VMEM((ticks, N - 1, T - 1, R, PW), low),
            pltpu.VMEM((ticks, T - 1, R, PW), low), pltpu.VMEM((ticks, T - 1, R, PW), low),
            pltpu.VMEM((ticks, TOK, PW), low),
            pltpu.VMEM((ticks, TOK, PW), low), pltpu.VMEM((ticks, N, T, R, PW), low),
            pltpu.VMEM((ticks, N - 1, T, R, BW), low), pltpu.VMEM((ticks, N - 1, T - 1, R, BW), low),
            pltpu.VMEM((ticks, N - 1, R, BW), low), pltpu.VMEM((ticks, N - 1, R, BW), low), pltpu.VMEM((ticks, R, BW), wide),
            pltpu.VMEM((N, R, BW), wide),
            pltpu.VMEM((BW, PW), wide), pltpu.VMEM((T - 1, BW, PW), low), pltpu.VMEM((T - 1, BW, PW), low),
            pltpu.VMEM((R, D), low), pltpu.VMEM((R, D), low), pltpu.VMEM((R, D), low), pltpu.VMEM(q.shape, low),
            pltpu.VMEM((BW, 2, PW // 2), low),
            pltpu.VMEM((ticks, 2, TOK * q.shape[-1] // (PW // 2), PW // 2), low),
            pltpu.VMEM((ticks, TOK * q.shape[-1] // (PW // 2), TOK), low),
            dma((6,)), dma((N,)), dma((T - 1, 2)), dma((T - 1, 2)),
            dma((ticks, 2, N - 1)), dma((ticks, 2, N - 1)), dma((T - 1, 2)), dma((T - 1, 2)),
            dma((ticks, N - 1)), dma((ticks, N - 1)), dma((ticks, T - 1)), dma((ticks, T - 1)),
            dma((ticks, T - 1)), dma((ticks, T - 1)), dma((4, N - 1)), dma((4, N - 1)),
            dma((ticks, N - 1, T - 1)), dma((ticks, N - 1, T - 1)), dma((ticks, N - 1)), dma((ticks, N - 1)),
            dma((T - 1, Q)), dma((T - 1, Q)), dma((1,)), dma((1,)),
        ],
        compiler_params=pltpu.CompilerParams(
            collective_id=0, has_side_effects=True, vmem_limit_bytes=62_000_000
        ),
    )(
        x, norm_gain, projection.reshape(D, 2, PW // 2), q, og, section_cotangent[0, 0], loss_cotangent[0],
        lengths.reshape(ticks), segments[0, 0],
    )
    query_grad, residual_grad, projection_grad = settle(outs)
    return (
        query_grad[None, None, :, :, None, :],
        residual_grad[None, None],
        projection_grad.reshape(1, BW, 1, 2, PW // 2),
    )


def solution(mesh):
    in_specs = (
        P("section", "dp", None, "tensor", None),
        P("section", None),
        P("section", None, "tensor", None, None),
        P("section", "dp", None, None, "tensor", None),
        P("section", "dp", None, None, "tensor", None),
        P("section", "dp", "tensor", None),
        P("dp", "tensor", None),
        P("section", "dp", None),
        P("section", "dp", None, None),
    )
    out_specs = (
        P("section", "dp", None, None, "tensor", None),
        P("section", "dp", "tensor", None),
        P("section", "dp", "tensor", None, None),
    )
    return jax.shard_map(on_device, mesh=mesh, in_specs=in_specs, out_specs=out_specs, check_vma=False)
```
